256 devices in a mesh: gx: 16 (over z_hi, x, core), ev: 16 (over y, z_lo).
Axes of the slice: x: 4, y: 4, z: 8 (z_hi: 2, z_lo: 4; z = z_hi * 4 + z_lo), core: 2. Of those that a mesh axis runs over, the one named last changes fastest.
Arguments:
- partial_kernels: bfloat16 [16, 2048, 2, 8, 2048], P('ev', 'gx'), may hold values from -8 to 8
- illumination: float32 [2048, 8, 2048], P('gx', None, 'ev'), may hold values from 0.3 to 3
- classes_x: int32 [8, 2048], P(None, 'ev'), may hold values from 0 to 2
- classes_y: int32 [2048, 8], P('gx'), may hold values from 0 to 2
- widths_x: float32 [3], replicated, may hold values from 0.5 to 1
- widths_y: float32 [3], replicated, may hold values from 0.5 to 1
Outputs:
- conditioned: bfloat16 [2048, 2, 8, 2048], P('gx', None, None, 'ev')
The draws below stay inside these ranges and needn't reach their ends.
All inputs are finite; a program needn't handle non-finite values.
Results may differ from the reference program's by a relative error of at most 0.0035.
Values may be sent and summed in bfloat16 or wider, within the bound.
A program may use at most 192 MiB of HBM per device.

```python
import math
import jax
import jax.numpy as jnp
from jax import lax

NX = 2048
NY = 2048
KERNELS = 2
NZ = 8
CLASSES = 3
BAND = 128
GROUPS = 16


def draw_partial_kernels(key, part):
    streams = jax.random.split(key, 6)
    extent = (GROUPS, NX, KERNELS, NZ, NY)
    per_map = (GROUPS, 1, KERNELS, NZ, 1)
    noise_part = jnp.clip(jax.random.normal(streams[0], extent, jnp.float32), -5.0, 5.0)
    wave_x = jax.random.randint(streams[1], per_map, 1, 4).astype(jnp.float32)
    wave_y = jax.random.randint(streams[2], per_map, 1, 4).astype(jnp.float32)
    phase_x = jax.random.uniform(streams[3], per_map, jnp.float32, 0.0, 2.0 * math.pi)
    phase_y = jax.random.uniform(streams[4], per_map, jnp.float32, 0.0, 2.0 * math.pi)
    height = jax.random.uniform(streams[5], per_map, jnp.float32, 0.5, 1.5)
    grid_x = (jnp.arange(NX, dtype=jnp.float32) / NX).reshape(1, NX, 1, 1, 1)
    grid_y = (jnp.arange(NY, dtype=jnp.float32) / NY).reshape(1, 1, 1, 1, NY)
    smooth = height * jnp.cos(2.0 * math.pi * wave_x * grid_x + phase_x) * jnp.cos(2.0 * math.pi * wave_y * grid_y + phase_y)
    return (noise_part + 1.5 * smooth).astype(jnp.bfloat16)


def touch_ends(values, own_key, smallest, top_value):
    shape = values.shape
    index_at = [jax.random.randint(jax.random.fold_in(own_key, axis), (), 0, shape[axis]) for axis in range(len(shape))]
    values = values.at[tuple(index_at)].set(smallest)
    longest = shape.index(max(shape))
    index_at[longest] = (index_at[longest] + 1) % shape[longest]
    return values.at[tuple(index_at)].set(top_value)


def block_levels(stream_key, shape, cuts, least, top_value):
    gain, own = 1.0, jax.random.fold_in(stream_key, 6)
    for position, shards_of in cuts:
        heights = jnp.exp(jax.random.uniform(jax.random.fold_in(own, position), (shards_of,), jnp.float32, least / len(cuts), top_value / len(cuts)))
        gain = gain * jnp.repeat(heights, shape[position] // shards_of).reshape([-1 if axis == position else 1 for axis in range(len(shape))])
    return gain


def setup_inputs(seed: int = 0) -> dict:
    key_list = jax.random.split(jax.random.key(seed), 7)
    return {
        "partial_kernels": draw_partial_kernels(jax.random.fold_in(key_list[6], 71), 0),
        "illumination": jnp.clip(jnp.exp(math.log(3.0) - 2.3025851 * jax.random.uniform(key_list[1], (NX, NZ, NY), jnp.float32) ** block_levels(key_list[1], (NX, NZ, NY), ((0, 16), (2, 16)), -0.2, 0.2)), 0.3, 3.0),
        "classes_x": touch_ends(jax.random.randint(key_list[2], (NZ, NY), 0, CLASSES), jax.random.fold_in(key_list[2], 1), 0, CLASSES - 1).astype(jnp.int32),
        "classes_y": touch_ends(jax.random.randint(key_list[3], (NX, NZ), 0, CLASSES), jax.random.fold_in(key_list[3], 1), 0, CLASSES - 1).astype(jnp.int32),
        "widths_x": jnp.clip(jnp.exp(jax.random.uniform(key_list[4], (CLASSES,), jnp.float32, math.log(0.5), math.log(1.0))), 0.5, 1.0),
        "widths_y": jnp.clip(jnp.exp(jax.random.uniform(key_list[5], (CLASSES,), jnp.float32, math.log(0.5), math.log(1.0))), 0.5, 1.0),
    }


blend_weight = 0.25
soft_bound = 2.0


def smoother(length, fraction):
    positions = jnp.arange(length, dtype=jnp.float32)
    offset = positions[:, None] - positions[None, :]
    distance = offset / (fraction * BAND)
    gaussian = jnp.where(jnp.abs(offset) <= BAND, jnp.exp(-0.5 * distance * distance), jnp.float32(0.0))
    gaussian = gaussian / jnp.sum(gaussian, axis=1, keepdims=True)
    return (gaussian + blend_weight * jnp.eye(length, dtype=jnp.float32)).astype(jnp.bfloat16)


def smooth_columns(columns, labels, matrices):
    summed = jnp.zeros((matrices[0].shape[0], columns.shape[1]), jnp.float32)
    for level in range(len(matrices)):
        product = jnp.dot(matrices[level], columns, preferred_element_type=jnp.float32)
        summed = summed + jnp.where(labels[None, :] == level, product, jnp.float32(0.0))
    return summed


def smooth_rows(row_block, labels, matrices):
    summed = jnp.zeros((row_block.shape[0], matrices[0].shape[0]), jnp.float32)
    for level in range(len(matrices)):
        product = lax.dot_general(row_block, matrices[level], (((1,), (1,)), ((), ())), preferred_element_type=jnp.float32)
        summed = summed + jnp.where(labels[:, None] == level, product, jnp.float32(0.0))
    return summed


def reference(partial_kernels, illumination, classes_x, classes_y, widths_x, widths_y):
    def accumulate(summed, group_term):
        return summed + group_term.astype(jnp.float32), None

    summed, unused = lax.scan(accumulate, jnp.zeros(partial_kernels.shape[1:], jnp.float32), partial_kernels)
    scaled = (summed / illumination[:, None, :, :]).astype(jnp.bfloat16)
    matrices_x = [smoother(NX, widths_x[level]) for level in range(CLASSES)]
    matrices_y = [smoother(NY, widths_y[level]) for level in range(CLASSES)]
    flattened = scaled.reshape(NX, KERNELS * NZ * NY)
    col_class = jnp.broadcast_to(classes_x[None, :, :], (KERNELS, NZ, NY)).reshape(-1)
    smoothed_x = smooth_columns(flattened, col_class, matrices_x)
    bounded = (soft_bound * jnp.tanh(smoothed_x / soft_bound)).astype(jnp.bfloat16)
    row_block = bounded.reshape(NX * KERNELS * NZ, NY)
    row_class = jnp.broadcast_to(classes_y[:, None, :], (NX, KERNELS, NZ)).reshape(-1)
    smoothed_y = smooth_rows(row_block, row_class, matrices_y)
    return smoothed_y.astype(jnp.bfloat16).reshape(NX, KERNELS, NZ, NY)
```

```python
import functools

import jax
import jax.numpy as jnp
from jax import lax
from jax.experimental import pallas as pl
from jax.experimental.pallas import tpu as pltpu
from jax.sharding import PartitionSpec as P

BAND = 128
blend_weight = 0.25
soft_bound = 2.0
MESH = pl.DeviceIdType.MESH
bf16, f32 = jnp.bfloat16, jnp.float32

RING = 4
LINE = 4
CHUNKS = ((0, 0, 64), (0, 64, 64), (1, 0, 64), (1, 64, 32), (1, 96, 32))
HALVES = 2
LINE_DTYPE = jnp.bfloat16
SEMS = 200


def window(first, length, fraction, along_rows, i, j):
    offset = (i + BAND - j).astype(f32)
    source = first - BAND + j
    inside = (jnp.abs(offset) <= BAND) & (source >= 0) & (source < length)
    distance = offset / (fraction * BAND)
    gaussian = jnp.where(inside, jnp.exp(-0.5 * distance * distance), 0.0)
    gaussian = gaussian / jnp.sum(gaussian, axis=along_rows, keepdims=True)
    return (gaussian + jnp.where(offset == 0.0, blend_weight, 0.0)).astype(bf16)


def kernel(
    sizes, x_hbm, ill_ref, cx_ref, cy_ref, wx_ref, wy_ref, out_ref,
    own, nxt, got, ym, yp, left, right, line, cells, xe, be, mx, my, cyt, sem,
):
    owners, groups = sizes
    slab, kernels, planes, full_y = x_hbm.shape
    block = full_y // groups
    span = block * LINE
    count = mx.shape[0] // slab
    g, e = lax.axis_index("gx"), lax.axis_index("ev")
    y, z = lax.div(e, LINE), lax.rem(e, LINE)
    up, down, across = (lax.rem(y + d, RING) for d in (1, RING - 1, 2))
    e_up, e_down = up * LINE + z, down * LINE + z

    index = {}

    def s(*key):
        return sem.at[index.setdefault(key, len(index))]

    drains = []

    def send(src, dst, name, to, cond=None):
        def make():
            return pltpu.make_async_remote_copy(
                src_ref=src(), dst_ref=dst(), send_sem=s("send", *name), recv_sem=s("recv", *name),
                device_id=to, device_id_type=MESH,
            )

        if cond is None:
            make().start()
        else:
            pl.when(cond)(lambda: make().start())
        drains.append((cond, lambda: make().wait_send()))

    def await_recv(dst, name, cond=None):
        def wait():
            pltpu.make_async_copy(dst, dst, s("recv", *name)).wait()

        if cond is None:
            wait()
        else:
            pl.when(cond)(wait)

    barrier = pltpu.get_barrier_semaphore()
    pl.semaphore_signal(barrier, inc=1, device_id={"ev": e_up}, device_id_type=MESH)
    pl.semaphore_signal(barrier, inc=1, device_id={"ev": e_down}, device_id_type=MESH)
    peers = 2
    for cond, to in (
        (e < groups - 1, {"ev": e + 1}),
        (e > 0, {"ev": e - 1}),
        (g < owners - 1, {"gx": g + 1}),
        (g > 0, {"gx": g - 1}),
    ):
        pl.when(cond)(
            functools.partial(pl.semaphore_signal, barrier, inc=1, device_id=to, device_id_type=MESH)
        )
        peers = peers + cond.astype(jnp.int32)
    pl.semaphore_wait(barrier, peers)

    def cols(target):
        return pl.ds(pl.multiple_of(target * span, span), span)

    def send_across(c):
        k, x0, n = CHUNKS[c]
        h = n // 2
        lo, hi = pl.ds(x0, h), pl.ds(x0 + h, h)
        send(lambda: x_hbm.at[lo, k, :, cols(across)], lambda: got.at[k, lo], ("a+", c), {"ev": e_up})
        send(lambda: x_hbm.at[hi, k, :, cols(across)], lambda: got.at[k, hi], ("a-", c), {"ev": e_down})

    def send_raw(c):
        k, x0, n = CHUNKS[c]
        h = n // 2
        lo, hi = pl.ds(x0, h), pl.ds(x0 + h, h)
        send(lambda: x_hbm.at[hi, k, :, cols(up)], lambda: ym.at[k, hi], ("r+", c), {"ev": e_up})
        send(lambda: x_hbm.at[lo, k, :, cols(down)], lambda: yp.at[k, lo], ("r-", c), {"ev": e_down})

    def loads(c):
        k, x0, n = CHUNKS[c]
        h = n // 2
        lo, hi, rows = pl.ds(x0, h), pl.ds(x0 + h, h), pl.ds(x0, n)
        return (
            pltpu.make_async_copy(x_hbm.at[lo, k, :, cols(up)], nxt.at[k, lo], s("nxt+", c)),
            pltpu.make_async_copy(x_hbm.at[hi, k, :, cols(down)], nxt.at[k, hi], s("nxt-", c)),
            pltpu.make_async_copy(x_hbm.at[rows, k, :, cols(y)], own.at[k, rows], s("own", c)),
        )

    def ring_stage(c):
        k, x0, n = CHUNKS[c]
        h = n // 2
        lo, hi = pl.ds(x0, h), pl.ds(x0 + h, h)
        for copy in loads(c)[:2]:
            copy.wait()
        await_recv(got.at[k, lo], ("a+", c))
        await_recv(got.at[k, hi], ("a-", c))

        def add(t, carry):
            r = pl.ds(x0 + 4 * t, 4)
            nxt[k, r] = (nxt[k, r].astype(f32) + got[k, r].astype(f32)).astype(bf16)
            return carry

        lax.fori_loop(0, n // 4, add, 0)
        send(lambda: nxt.at[k, lo], lambda: ym.at[k, lo], ("s+", c), {"ev": e_up})
        send(lambda: nxt.at[k, hi], lambda: yp.at[k, hi], ("s-", c), {"ev": e_down})

    def ring_done(c):
        k, x0, n = CHUNKS[c]
        h = n // 2
        lo, hi = pl.ds(x0, h), pl.ds(x0 + h, h)
        loads(c)[2].wait()
        await_recv(ym.at[k, hi], ("r+", c))
        await_recv(yp.at[k, lo], ("r-", c))
        await_recv(ym.at[k, lo], ("s+", c))
        await_recv(yp.at[k, hi], ("s-", c))

    def unit(c, target, rightward, first, slot):
        k, x0, n = CHUNKS[c]
        lanes = pl.ds(target * block, block)
        arrived = left if rightward else right
        name = ("l" if rightward else "r", c, target)
        rows = pl.ds(x0, n)
        if not first:
            await_recv(arrived.at[k, rows, :, lanes], name)

        def add(t, carry):
            r = pl.ds(x0 + 8 * t, 8)
            total = own[k, r, :, lanes].astype(f32) + ym[k, r, :, lanes].astype(f32)
            total = total + yp[k, r, :, lanes].astype(f32)
            if not first:
                total = total + arrived[k, r, :, lanes].astype(f32)
            line[k, r, :, lanes] = total.astype(line.dtype)
            return carry

        lax.fori_loop(0, n // 8, add, 0)
        make = lambda: pltpu.make_async_remote_copy(
            src_ref=line.at[k, rows, :, lanes], dst_ref=arrived.at[k, rows, :, lanes],
            send_sem=s("linesend", c, slot), recv_sem=s("recv", *name),
            device_id={"ev": e + 1 if rightward else e - 1}, device_id_type=MESH,
        )
        make().start()
        return lambda: make().wait_send()

    line_drains = {at: [] for at in range(LINE)}

    def line_stage(c, plan):
        for at, units in plan.items():
            def run(at=at, units=units):
                for target, rightward, first, slot in units:
                    line_drains[at].append(unit(c, target, rightward, first, slot))
            pl.when(z == at)(run)

    hop0 = {0: [(t, True, True, 3 - t) for t in (3, 2, 1)], 3: [(t, False, True, t) for t in (0, 1, 2)]}
    hop1 = {1: [(3, True, False, 0), (2, True, False, 1)], 2: [(0, False, False, 0), (1, False, False, 1)]}
    hop2 = {2: [(3, True, False, 2)], 1: [(0, False, False, 2)]}

    def finish(c):
        k, x0, n = CHUNKS[c]
        rows = pl.ds(x0, n)
        lanes = pl.ds(pl.multiple_of(z * block, block), block)
        for at in range(LINE):
            here = pl.ds(at * block, block)
            if at > 0:
                await_recv(left.at[k, rows, :, here], ("l", c, at), z == at)
            if at < LINE - 1:
                await_recv(right.at[k, rows, :, here], ("r", c, at), z == at)

        def add(t, carry):
            r = pl.ds(x0 + 8 * t, 8)
            total = own[k, r, :, lanes].astype(f32) + ym[k, r, :, lanes].astype(f32)
            total = total + yp[k, r, :, lanes].astype(f32)
            total = total + left[k, r, :, lanes].astype(f32) + right[k, r, :, lanes].astype(f32)
            cells[pl.ds(64 * t, 64), :] = (total / ill_ref[r]).reshape(8 * planes, block)
            return carry

        lax.fori_loop(0, n // 8, add, 0)
        for plane in range(planes):
            xe[k, plane, pl.ds(slab + x0, n), :] = cells[pl.ds(plane, n, stride=planes), :].astype(bf16)
        src = lambda: xe.at[k, :, pl.ds(slab + x0, n), :]
        send(src, lambda: xe.at[k, :, pl.ds(x0, n), :], ("x+", c), {"gx": g + 1}, g < owners - 1)
        send(src, lambda: xe.at[k, :, pl.ds(2 * slab + x0, n), :], ("x-", c), {"gx": g - 1}, g > 0)

    def smooth_x(k):
        for c, (kc, x0, n) in enumerate(CHUNKS):
            if kc == k:
                await_recv(xe.at[k, :, pl.ds(x0, n), :], ("x+", c), g > 0)
                await_recv(xe.at[k, :, pl.ds(2 * slab + x0, n), :], ("x-", c), g < owners - 1)
        step = planes // HALVES
        for half in range(HALVES):
            def pair(t, carry, half=half):
                p = half * step + 2 * t
                data = jnp.concatenate([xe[k, p], xe[k, p + 1]], axis=1)
                labels = jnp.concatenate([cx_ref[pl.ds(p, 1), :], cx_ref[pl.ds(p + 1, 1), :]], axis=1)
                product = jnp.dot(mx[...], data, preferred_element_type=f32)
                total = product[:slab]
                for level in range(1, count):
                    total = jnp.where(labels == level, product[level * slab : (level + 1) * slab], total)
                bounded = (soft_bound * jnp.tanh(total / soft_bound)).astype(bf16)
                be[k, 1, p] = bounded[:, :block]
                be[k, 1, p + 1] = bounded[:, block:]
                return carry

            lax.fori_loop(0, step // 2, pair, 0)
            part = pl.ds(half * step, step)
            src = lambda part=part: be.at[k, 1, part]
            send(src, lambda part=part: be.at[k, 0, part], ("y+", k, half), {"ev": e + 1}, e < groups - 1)
            send(src, lambda part=part: be.at[k, 2, part], ("y-", k, half), {"ev": e - 1}, e > 0)

    def smooth_y(k):
        step = planes // HALVES
        for half in range(HALVES):
            part = pl.ds(half * step, step)
            await_recv(be.at[k, 0, part], ("y+", k, half), e > 0)
            await_recv(be.at[k, 2, part], ("y-", k, half), e < groups - 1)

            def pair(t, carry, half=half):
                p = half * step + 2 * t
                two = pl.ds(p, 2)
                data = jnp.concatenate([be[k, side, two].reshape(2 * slab, block) for side in range(3)], axis=1)
                product = jnp.dot(data, my[...], preferred_element_type=f32)
                labels = cyt[two].reshape(2 * slab, block)
                total = product[:, :block]
                for level in range(1, count):
                    total = jnp.where(labels == level, product[:, level * block : (level + 1) * block], total)
                out_ref[k, two] = total.astype(out_ref.dtype).reshape(2, slab, block)
                return carry

            lax.fori_loop(0, step // 2, pair, 0)

    def prepare():
        i = lax.broadcasted_iota(jnp.int32, (slab, slab + 2 * BAND), 0)
        j = lax.broadcasted_iota(jnp.int32, (slab, slab + 2 * BAND), 1)
        for level in range(count):
            mx[level * slab : (level + 1) * slab, :] = window(g * slab, slab * owners, wx_ref[level], 1, i, j)
        j = lax.broadcasted_iota(jnp.int32, (block + 2 * BAND, block), 0)
        i = lax.broadcasted_iota(jnp.int32, (block + 2 * BAND, block), 1)
        for level in range(count):
            my[:, level * block : (level + 1) * block] = window(e * block, full_y, wy_ref[level], 0, i, j)
        for plane in range(planes):
            row = cy_ref[plane : plane + 1, :].astype(f32)
            cyt[plane] = jnp.broadcast_to(row, (slab, slab)).T

        def zero(ref):
            def fill():
                ref[...] = jnp.zeros(ref.shape, ref.dtype)
            return fill

        pl.when(z == 0)(zero(left.at[:, :, :, pl.ds(0, block)]))
        pl.when(z == LINE - 1)(zero(right.at[:, :, :, pl.ds((LINE - 1) * block, block)]))
        pl.when(g == 0)(zero(xe.at[:, :, pl.ds(0, slab), :]))
        pl.when(g == owners - 1)(zero(xe.at[:, :, pl.ds(2 * slab, slab), :]))
        pl.when(e == 0)(zero(be.at[:, 0]))
        pl.when(e == groups - 1)(zero(be.at[:, 2]))

    total_chunks = len(CHUNKS)
    send_across(0)
    send_raw(0)
    send_across(1)
    for c in range(total_chunks):
        for copy in loads(c):
            copy.start()
    prepare()
    ready = {}
    for k in range(kernels):
        ready[k] = max(c for c in range(total_chunks) if CHUNKS[c][0] == k) + 3
    for slot in range(total_chunks + 4):
        if slot < total_chunks:
            ring_stage(slot)
            if slot + 1 < total_chunks:
                send_raw(slot + 1)
            if slot + 2 < total_chunks:
                send_across(slot + 2)
        if 0 <= slot - 1 < total_chunks:
            ring_done(slot - 1)
            line_stage(slot - 1, hop0)
        if 0 <= slot - 2 < total_chunks:
            line_stage(slot - 2, hop2)
            finish(slot - 2)
        if 0 <= slot - 1 < total_chunks:
            line_stage(slot - 1, hop1)
        for k in range(kernels):
            if slot == ready[k]:
                smooth_x(k)
            if slot == ready[k] + 1:
                smooth_y(k)

    for cond, drain in drains:
        if cond is None:
            drain()
        else:
            pl.when(cond)(drain)
    for at, waits in line_drains.items():
        def run(waits=waits):
            for wait in waits:
                wait()
        pl.when(z == at)(run)
    assert len(index) <= SEMS


def per_device(partial_kernels, illumination, classes_x, classes_y, widths_x, widths_y):
    own_part = partial_kernels[0]
    slab, kernels, planes, full_y = own_part.shape
    groups, owners = lax.axis_size("ev"), lax.axis_size("gx")
    block = full_y // groups
    span = block * LINE
    count = widths_x.shape[0]
    vmem, smem = pl.BlockSpec(memory_space=pltpu.VMEM), pl.BlockSpec(memory_space=pltpu.SMEM)
    wide = (kernels, slab, planes, span)
    out = pl.pallas_call(
        functools.partial(kernel, (owners, groups)),
        out_shape=jax.ShapeDtypeStruct((kernels, planes, slab, block), bf16),
        in_specs=[pl.BlockSpec(memory_space=pl.ANY), vmem, vmem, vmem, smem, smem],
        out_specs=vmem,
        scratch_shapes=[
            pltpu.VMEM(wide, bf16),
            pltpu.VMEM(wide, bf16),
            pltpu.VMEM(wide, bf16),
            pltpu.VMEM(wide, bf16),
            pltpu.VMEM(wide, bf16),
            pltpu.VMEM(wide, LINE_DTYPE),
            pltpu.VMEM(wide, LINE_DTYPE),
            pltpu.VMEM(wide, LINE_DTYPE),
            pltpu.VMEM((64 * planes, block), f32),
            pltpu.VMEM((kernels, planes, 3 * slab, block), bf16),
            pltpu.VMEM((kernels, 3, planes, slab, block), bf16),
            pltpu.VMEM((count * slab, slab + 2 * BAND), bf16),
            pltpu.VMEM((block + 2 * BAND, count * block), bf16),
            pltpu.VMEM((planes, slab, slab), f32),
            pltpu.SemaphoreType.DMA((SEMS,)),
        ],
        compiler_params=pltpu.CompilerParams(
            collective_id=0, has_side_effects=True, vmem_limit_bytes=56 * 1024 * 1024
        ),
        cost_estimate=pl.CostEstimate(flops=2_000_000_000, bytes_accessed=16_000_000, transcendentals=300_000),
        name="condition",
    )(own_part, illumination, classes_x, classes_y.T, widths_x, widths_y)
    return out.transpose(2, 0, 1, 3)


def solution(mesh):
    return jax.shard_map(
        per_device,
        mesh=mesh,
        in_specs=(
            P("ev", "gx", None, None, None),
            P("gx", None, "ev"),
            P(None, "ev"),
            P("gx", None),
            P(),
            P(),
        ),
        out_specs=P("gx", None, None, "ev"),
        check_vma=False,
    )
```

```python
import functools

import jax
import jax.numpy as jnp
from jax import lax
from jax.experimental import pallas as pl
from jax.experimental.pallas import tpu as pltpu
from jax.sharding import PartitionSpec as P

BAND = 128
blend_weight = 0.25
soft_bound = 2.0
MESH = pl.DeviceIdType.MESH
bf16, f32 = jnp.bfloat16, jnp.float32

RING = 4
LINE = 4
PLANES = 4
CHUNKS = ((0, 0, 32), (0, 32, 32), (1, 0, 32), (1, 32, 32), (2, 0, 32), (2, 32, 32), (3, 0, 32), (3, 32, 16), (3, 48, 16))
SEMS = 320


def window(first, length, fraction, along_rows, i, j):
    offset = (i + BAND - j).astype(f32)
    source = first - BAND + j
    inside = (jnp.abs(offset) <= BAND) & (source >= 0) & (source < length)
    distance = offset / (fraction * BAND)
    gaussian = jnp.where(inside, jnp.exp(-0.5 * distance * distance), 0.0)
    gaussian = gaussian / jnp.sum(gaussian, axis=along_rows, keepdims=True)
    return (gaussian + jnp.where(offset == 0.0, blend_weight, 0.0)).astype(bf16)


def kernel(
    sizes, x_hbm, ill_hbm, cx_ref, cy_ref, wx_ref, wy_ref, out_ref,
    own, nxt, got, ym, yp, left16, right16, line16, left32, right32, line32, ill, cells, xe, be, mx, my, cyt, sem,
):
    owners, groups = sizes
    slab, kernels, planes, full_y = x_hbm.shape
    block = full_y // groups
    span = block * LINE
    half = slab // 2
    count = mx.shape[0] // slab
    per_kernel = planes // PLANES
    pieces = kernels * per_kernel
    g, e = lax.axis_index("gx"), lax.axis_index("ev")
    y, z = lax.div(e, LINE), lax.rem(e, LINE)
    up, down, across = (lax.rem(y + d, RING) for d in (1, RING - 1, 2))
    e_up, e_down = up * LINE + z, down * LINE + z

    index = {}

    def s(*key):
        return sem.at[index.setdefault(key, len(index))]

    drains = []

    def when(cond, action):
        if cond is None:
            action()
        else:
            pl.when(cond)(action)

    def send(src, dst, name, to, cond=None):
        def make():
            return pltpu.make_async_remote_copy(
                src_ref=src(), dst_ref=dst(), send_sem=s("send", *name), recv_sem=s("recv", *name),
                device_id=to, device_id_type=MESH,
            )

        when(cond, lambda: make().start())
        drains.append((cond, lambda: make().wait_send()))

    def await_recv(dst, name, cond=None):
        when(cond, lambda: pltpu.make_async_copy(dst, dst, s("recv", *name)).wait())

    barrier = pltpu.get_barrier_semaphore()
    pl.semaphore_signal(barrier, inc=1, device_id={"ev": e_up}, device_id_type=MESH)
    pl.semaphore_signal(barrier, inc=1, device_id={"ev": e_down}, device_id_type=MESH)
    peers = 2
    for cond, to in (
        (e < groups - 1, {"ev": e + 1}),
        (e > 0, {"ev": e - 1}),
        (g < owners - 1, {"gx": g + 1}),
        (g > 0, {"gx": g - 1}),
    ):
        pl.when(cond)(
            functools.partial(pl.semaphore_signal, barrier, inc=1, device_id=to, device_id_type=MESH)
        )
        peers = peers + cond.astype(jnp.int32)
    pl.semaphore_wait(barrier, peers)

    def term(chunk, side, target):
        p, r0, n = chunk
        lanes = pl.ds(pl.multiple_of(target * span, span), span)
        first = (p % per_kernel) * PLANES
        return x_hbm.at[pl.ds(side * half + r0, n), p // per_kernel, pl.ds(first, PLANES), lanes]

    def part(ref, chunk, side):
        p, r0, n = chunk
        return ref.at[p, pl.ds(r0, n), pl.ds(side * PLANES, PLANES), :]

    def send_across(c):
        chunk = CHUNKS[c]
        send(lambda: term(chunk, 0, across), lambda: part(got, chunk, 0), ("a+", c), {"ev": e_up})
        send(lambda: term(chunk, 1, across), lambda: part(got, chunk, 1), ("a-", c), {"ev": e_down})

    def send_raw(c):
        chunk = CHUNKS[c]
        send(lambda: term(chunk, 1, up), lambda: part(ym, chunk, 1), ("r+", c), {"ev": e_up})
        send(lambda: term(chunk, 0, down), lambda: part(yp, chunk, 0), ("r-", c), {"ev": e_down})

    def loads(c):
        chunk = CHUNKS[c]
        for side, ref, target, name in (
            (0, nxt, up, "n0"), (1, nxt, down, "n1"), (0, own, y, "o0"), (1, own, y, "o1"),
        ):
            yield name, lambda side=side, ref=ref, target=target, name=name: pltpu.make_async_copy(
                term(chunk, side, target), part(ref, chunk, side), s(name, c)
            )

    def ring_stage(c):
        chunk = p, r0, n = CHUNKS[c]
        for name, make in loads(c):
            if name[0] == "n":
                make().wait()
        await_recv(part(got, chunk, 0), ("a+", c))
        await_recv(part(got, chunk, 1), ("a-", c))

        def add(t, carry):
            r = pl.ds(r0 + 4 * t, 4)
            nxt[p, r] = (nxt[p, r].astype(f32) + got[p, r].astype(f32)).astype(bf16)
            return carry

        lax.fori_loop(0, n // 4, add, 0)
        send(lambda: part(nxt, chunk, 0), lambda: part(ym, chunk, 0), ("s+", c), {"ev": e_up})
        send(lambda: part(nxt, chunk, 1), lambda: part(yp, chunk, 1), ("s-", c), {"ev": e_down})

    def ring_done(c):
        chunk = CHUNKS[c]
        for name, make in loads(c):
            if name[0] == "o":
                make().wait()
        await_recv(part(ym, chunk, 1), ("r+", c))
        await_recv(part(yp, chunk, 0), ("r-", c))
        await_recv(part(ym, chunk, 0), ("s+", c))
        await_recv(part(yp, chunk, 1), ("s-", c))

    def unit(c, at, target, slot):
        p, r0, n = CHUNKS[c]
        rightward = target > at
        first = at == (0 if rightward else LINE - 1)
        lanes = pl.ds(target * block, block)
        rows = pl.ds(r0, n)
        name = ("l" if rightward else "r", c, target)

        def landing(source):
            short = source in (0, LINE - 1) and abs(target - source) > 1
            if rightward:
                return left16 if short else left32
            return right16 if short else right32

        arrived = landing(at - 1 if rightward else at + 1)
        to = landing(at)
        staged = line16 if to.dtype == bf16 else line32
        if not first:
            await_recv(arrived.at[p, rows, :, lanes], name)

        def add(t, carry):
            r = pl.ds(r0 + 8 * t, 8)
            total = own[p, r, :, lanes].astype(f32) + ym[p, r, :, lanes].astype(f32)
            total = total + yp[p, r, :, lanes].astype(f32)
            if not first:
                total = total + arrived[p, r, :, lanes].astype(f32)
            staged[p, r, :, lanes] = total.astype(staged.dtype)
            return carry

        lax.fori_loop(0, n // 8, add, 0)
        make = lambda: pltpu.make_async_remote_copy(
            src_ref=staged.at[p, rows, :, lanes], dst_ref=to.at[p, rows, :, lanes],
            send_sem=s("linesend", c, slot), recv_sem=s("recv", *name),
            device_id={"ev": e + 1 if rightward else e - 1}, device_id_type=MESH,
        )
        make().start()
        return lambda: make().wait_send()

    line_drains = {at: [] for at in range(LINE)}

    def line_stage(c, plan):
        for at, units in plan.items():
            def run(at=at, units=units):
                for target, slot in units:
                    line_drains[at].append(unit(c, at, target, slot))
            pl.when(z == at)(run)

    hop0 = {0: [(3, 0), (2, 1), (1, 2)], 3: [(0, 0), (1, 1), (2, 2)]}
    hop1 = {1: [(3, 0), (2, 1)], 2: [(0, 0), (1, 1)]}
    hop2 = {2: [(3, 2)], 1: [(0, 2)]}

    def finish(c):
        p, r0, n = CHUNKS[c]
        zg = p % per_kernel
        rows = pl.ds(r0, n)
        lanes = pl.ds(pl.multiple_of(z * block, block), block)
        for at in range(LINE):
            here = pl.ds(at * block, block)
            if at > 0:
                await_recv(left32.at[p, rows, :, here], ("l", c, at), z == at)
            if at < LINE - 1:
                await_recv(right32.at[p, rows, :, here], ("r", c, at), z == at)

        def add(t, carry):
            r = pl.ds(r0 + 8 * t, 8)
            total = own[p, r, :, lanes].astype(f32) + ym[p, r, :, lanes].astype(f32)
            total = total + yp[p, r, :, lanes].astype(f32)
            total = total + left32[p, r, :, lanes] + right32[p, r, :, lanes]
            cells[pl.ds(16 * PLANES * t, 16 * PLANES), :] = (total / ill[zg, r]).reshape(16 * PLANES, block)
            return carry

        lax.fori_loop(0, n // 8, add, 0)
        for side in range(2):
            for plane in range(PLANES):
                picked = cells[pl.ds(side * PLANES + plane, n, stride=2 * PLANES), :]
                xe[p, plane, 2 + side, rows, :] = picked.astype(bf16)
        src = lambda: xe.at[p, :, pl.ds(2, 2), rows, :]
        send(src, lambda: xe.at[p, :, pl.ds(0, 2), rows, :], ("x+", c), {"gx": g + 1}, g < owners - 1)
        send(src, lambda: xe.at[p, :, pl.ds(4, 2), rows, :], ("x-", c), {"gx": g - 1}, g > 0)

    def smooth_x(p):
        zg = p % per_kernel
        for c, (pc, r0, n) in enumerate(CHUNKS):
            if pc == p:
                await_recv(xe.at[p, :, pl.ds(0, 2), pl.ds(r0, n), :], ("x+", c), g > 0)
                await_recv(xe.at[p, :, pl.ds(4, 2), pl.ds(r0, n), :], ("x-", c), g < owners - 1)
        for a in range(0, PLANES, 2):
            data = jnp.concatenate([xe[p, b].reshape(3 * slab, block) for b in (a, a + 1)], axis=1)
            d = zg * PLANES + a
            labels = jnp.concatenate([cx_ref[d : d + 1, :], cx_ref[d + 1 : d + 2, :]], axis=1)
            product = jnp.dot(mx[...], data, preferred_element_type=f32)
            total = product[:slab]
            for level in range(1, count):
                total = jnp.where(labels == level, product[level * slab : (level + 1) * slab], total)
            bounded = (soft_bound * jnp.tanh(total / soft_bound)).astype(bf16)
            be[p, 1, a] = bounded[:, :block]
            be[p, 1, a + 1] = bounded[:, block:]
            two = pl.ds(a, 2)
            src = lambda two=two: be.at[p, 1, two]
            send(src, lambda two=two: be.at[p, 0, two], ("y+", p, a), {"ev": e + 1}, e < groups - 1)
            send(src, lambda two=two: be.at[p, 2, two], ("y-", p, a), {"ev": e - 1}, e > 0)

    def smooth_y(p):
        k, zg = p // per_kernel, p % per_kernel
        for a in range(0, PLANES, 2):
            two = pl.ds(a, 2)
            await_recv(be.at[p, 0, two], ("y+", p, a), e > 0)
            await_recv(be.at[p, 2, two], ("y-", p, a), e < groups - 1)
            data = jnp.concatenate([be[p, side, two].reshape(2 * slab, block) for side in range(3)], axis=1)
            product = jnp.dot(data, my[...], preferred_element_type=f32)
            deep = pl.ds(zg * PLANES + a, 2)
            labels = cyt[deep].reshape(2 * slab, block)
            total = product[:, :block]
            for level in range(1, count):
                total = jnp.where(labels == level, product[:, level * block : (level + 1) * block], total)
            out_ref[k, deep] = total.astype(out_ref.dtype).reshape(2, slab, block)

    def prepare():
        i = lax.broadcasted_iota(jnp.int32, (slab, slab + 2 * BAND), 0)
        j = lax.broadcasted_iota(jnp.int32, (slab, slab + 2 * BAND), 1)
        for level in range(count):
            mx[level * slab : (level + 1) * slab, :] = window(g * slab, slab * owners, wx_ref[level], 1, i, j)
        j = lax.broadcasted_iota(jnp.int32, (block + 2 * BAND, block), 0)
        i = lax.broadcasted_iota(jnp.int32, (block + 2 * BAND, block), 1)
        for level in range(count):
            my[:, level * block : (level + 1) * block] = window(e * block, full_y, wy_ref[level], 0, i, j)
        for plane in range(planes):
            row = cy_ref[plane : plane + 1, :].astype(f32)
            cyt[plane] = jnp.broadcast_to(row, (slab, slab)).T

        def zero(ref):
            def fill():
                ref[...] = jnp.zeros(ref.shape, ref.dtype)
            return fill

        pl.when(z == 0)(zero(left32.at[:, :, :, pl.ds(0, block)]))
        pl.when(z == LINE - 1)(zero(right32.at[:, :, :, pl.ds((LINE - 1) * block, block)]))
        pl.when(g == 0)(zero(xe.at[:, :, pl.ds(0, 2)]))
        pl.when(g == owners - 1)(zero(xe.at[:, :, pl.ds(4, 2)]))
        pl.when(e == 0)(zero(be.at[:, 0]))
        pl.when(e == groups - 1)(zero(be.at[:, 2]))

    def ill_loads():
        for zg in range(per_kernel):
            for side in range(2):
                yield lambda zg=zg, side=side: pltpu.make_async_copy(
                    ill_hbm.at[pl.ds(side * half, half), pl.ds(zg * PLANES, PLANES), :],
                    ill.at[zg, :, pl.ds(side * PLANES, PLANES), :], s("ill", zg, side),
                )

    chunks = len(CHUNKS)
    send_across(0)
    send_raw(0)
    send_across(1)
    for c in range(chunks):
        for name, make in loads(c):
            make().start()
    for make in ill_loads():
        make().start()
    ready = [max(c for c in range(chunks) if CHUNKS[c][0] == p) + 3 for p in range(pieces)]
    for slot in range(chunks + 4):
        if slot < chunks:
            ring_stage(slot)
            if slot + 1 < chunks:
                send_raw(slot + 1)
            if slot + 2 < chunks:
                send_across(slot + 2)
        if slot == 0:
            prepare()
            for make in ill_loads():
                make().wait()
        if 0 <= slot - 1 < chunks:
            ring_done(slot - 1)
            line_stage(slot - 1, hop0)
        if 0 <= slot - 2 < chunks:
            line_stage(slot - 2, hop2)
        if 0 <= slot - 1 < chunks:
            line_stage(slot - 1, hop1)
        if 0 <= slot - 2 < chunks:
            finish(slot - 2)
        for p in range(pieces):
            if slot == ready[p]:
                smooth_x(p)
        for p in range(pieces):
            if slot == (ready[-1] if p == pieces - 2 else ready[p] + (1 if p == pieces - 1 else 2)):
                smooth_y(p)

    for cond, drain in drains:
        when(cond, drain)
    for at, waits in line_drains.items():
        def run(waits=waits):
            for wait in waits:
                wait()
        pl.when(z == at)(run)
    assert len(index) <= SEMS, len(index)


def per_device(partial_kernels, illumination, classes_x, classes_y, widths_x, widths_y):
    own_part = partial_kernels[0]
    slab, kernels, planes, full_y = own_part.shape
    groups, owners = lax.axis_size("ev"), lax.axis_size("gx")
    block = full_y // groups
    span = block * LINE
    count = widths_x.shape[0]
    pieces = kernels * planes // PLANES
    vmem, smem = pl.BlockSpec(memory_space=pltpu.VMEM), pl.BlockSpec(memory_space=pltpu.SMEM)
    hbm = pl.BlockSpec(memory_space=pl.ANY)
    wide = (pieces, slab // 2, 2 * PLANES, span)
    out = pl.pallas_call(
        functools.partial(kernel, (owners, groups)),
        out_shape=jax.ShapeDtypeStruct((kernels, planes, slab, block), bf16),
        in_specs=[hbm, hbm, vmem, vmem, smem, smem],
        out_specs=vmem,
        scratch_shapes=[pltpu.VMEM(wide, bf16)] * 8
        + [pltpu.VMEM(wide, f32)] * 3
        + [
            pltpu.VMEM((planes // PLANES, slab // 2, 2 * PLANES, block), f32),
            pltpu.VMEM((slab * PLANES, block), f32),
            pltpu.VMEM((pieces, PLANES, 6, slab // 2, block), bf16),
            pltpu.VMEM((pieces, 3, PLANES, slab, block), bf16),
            pltpu.VMEM((count * slab, slab + 2 * BAND), bf16),
            pltpu.VMEM((block + 2 * BAND, count * block), bf16),
            pltpu.VMEM((planes, slab, slab), f32),
            pltpu.SemaphoreType.DMA((SEMS,)),
        ],
        compiler_params=pltpu.CompilerParams(
            collective_id=0, has_side_effects=True, vmem_limit_bytes=56 * 1024 * 1024
        ),
        cost_estimate=pl.CostEstimate(flops=2_000_000_000, bytes_accessed=16_000_000, transcendentals=300_000),
        name="condition",
    )(own_part, illumination, classes_x, classes_y.T, widths_x, widths_y)
    return out.transpose(2, 0, 1, 3)


def solution(mesh):
    return jax.shard_map(
        per_device,
        mesh=mesh,
        in_specs=(
            P("ev", "gx", None, None, None),
            P("gx", None, "ev"),
            P(None, "ev"),
            P("gx", None),
            P(),
            P(),
        ),
        out_specs=P("gx", None, None, "ev"),
        check_vma=False,
    )
```

```python
import functools

import jax
import jax.numpy as jnp
from jax import lax
from jax.experimental import pallas as pl
from jax.experimental.pallas import tpu as pltpu
from jax.sharding import PartitionSpec as P

BAND = 128
blend_weight = 0.25
soft_bound = 2.0
MESH = pl.DeviceIdType.MESH
bf16, f32 = jnp.bfloat16, jnp.float32

RING = 4
LINE = 4
PLANES = 4
CHUNKS = ((0,0,16),(0,16,48),(1,0,32),(1,32,32),(2,0,32),(2,32,32),(3,0,32),(3,32,32))
SEMS = 420


def window(first, length, fraction, along_rows, i, j):
    offset = (i + BAND - j).astype(f32)
    source = first - BAND + j
    inside = (jnp.abs(offset) <= BAND) & (source >= 0) & (source < length)
    distance = offset / (fraction * BAND)
    gaussian = jnp.where(inside, jnp.exp(-0.5 * distance * distance), 0.0)
    gaussian = gaussian / jnp.sum(gaussian, axis=along_rows, keepdims=True)
    return (gaussian + jnp.where(offset == 0.0, blend_weight, 0.0)).astype(bf16)


def kernel(
    sizes, x_hbm, ill_hbm, cx_ref, cy_ref, wx_ref, wy_ref, out_ref,
    own, nxt, got, ym, yp, via, via_out, near, near_out, far, far_out, ill, cells, xe, passed, be, mx, my, cyt, sem,
):
    owners, groups = sizes
    slab, kernels, planes, full_y = x_hbm.shape
    block = full_y // groups
    span = block * LINE
    half = slab // 2
    seam_hi = owners // 2
    seam_lo = seam_hi - 1
    count = mx.shape[0] // slab
    per_kernel = planes // PLANES
    pieces = kernels * per_kernel
    g, e = lax.axis_index("gx"), lax.axis_index("ev")
    y, z = lax.div(e, LINE), lax.rem(e, LINE)
    up, down, across = (lax.rem(y + d, RING) for d in (1, RING - 1, 2))
    e_up, e_down = up * LINE + z, down * LINE + z
    mate = z + 1 - 2 * lax.rem(z, 2)
    at_end = (z == 0) | (z == LINE - 1)
    inner = jnp.logical_not(at_end)

    def by_way(p):
        return 2 * p + 1, seam_hi + 2 * (p + 1)

    beyond = (lax.rem(z + 2, LINE), lax.rem(mate + 2, LINE))

    index = {}

    def s(*key):
        return sem.at[index.setdefault(key, len(index))]

    drains = []

    def when(cond, action):
        if cond is None:
            action()
        else:
            pl.when(cond)(action)

    def make_copy(src, dst, name, to, out=None):
        return pltpu.make_async_remote_copy(
            src_ref=src(), dst_ref=dst(), send_sem=s("send", *(out or name)), recv_sem=s("recv", *name),
            device_id=to, device_id_type=MESH,
        )

    def send(*copy, cond=None):
        when(cond, lambda: make_copy(*copy).start())
        drains.append((cond, lambda: make_copy(*copy).wait_send()))

    def await_recv(dst, name, cond=None):
        when(cond, lambda: pltpu.make_async_copy(dst, dst, s("recv", *name)).wait())

    barrier = pltpu.get_barrier_semaphore()
    pl.semaphore_signal(barrier, inc=1, device_id={"ev": e_up}, device_id_type=MESH)
    pl.semaphore_signal(barrier, inc=1, device_id={"ev": e_down}, device_id_type=MESH)
    pl.semaphore_signal(barrier, inc=1, device_id={"ev": y * LINE + beyond[0]}, device_id_type=MESH)
    peers = 3
    for cond, to in (
        (e < groups - 1, {"ev": e + 1}),
        (e > 0, {"ev": e - 1}),
        (g < owners - 1, {"gx": g + 1}),
        (g > 0, {"gx": g - 1}),
    ):
        pl.when(cond)(
            functools.partial(pl.semaphore_signal, barrier, inc=1, device_id=to, device_id_type=MESH)
        )
        peers = peers + cond.astype(jnp.int32)
    for p in range(pieces - 1):
        for at, to in (
            (by_way(p)[0], seam_lo), (seam_hi, by_way(p)[0]), (by_way(p)[1], seam_hi), (seam_lo, by_way(p)[1]),
        ):
            pl.when(g == at)(
                functools.partial(pl.semaphore_signal, barrier, inc=1, device_id={"gx": to}, device_id_type=MESH)
            )
            peers = peers + (g == to).astype(jnp.int32)

    def term(chunk, side, target):
        p, r0, n = chunk
        lanes = pl.ds(pl.multiple_of(target * span, span), span)
        first = (p % per_kernel) * PLANES
        return x_hbm.at[pl.ds(side * half + r0, n), p // per_kernel, pl.ds(first, PLANES), lanes]

    def part(ref, chunk, side):
        p, r0, n = chunk
        return ref.at[p, pl.ds(r0, n), pl.ds(side * PLANES, PLANES), :]

    def send_across(c):
        chunk = CHUNKS[c]
        send(lambda: term(chunk, 0, across), lambda: part(got, chunk, 0), ("a+", c), {"ev": e_up})
        send(lambda: term(chunk, 1, across), lambda: part(got, chunk, 1), ("a-", c), {"ev": e_down})

    def send_raw(c):
        chunk = CHUNKS[c]
        send(lambda: term(chunk, 1, up), lambda: part(ym, chunk, 1), ("r+", c), {"ev": e_up})
        send(lambda: term(chunk, 0, down), lambda: part(yp, chunk, 0), ("r-", c), {"ev": e_down})

    def loads(c):
        chunk = CHUNKS[c]
        for side, ref, target, name in (
            (0, nxt, up, "n0"), (1, nxt, down, "n1"), (0, own, y, "o0"), (1, own, y, "o1"),
        ):
            yield name, lambda side=side, ref=ref, target=target, name=name: pltpu.make_async_copy(
                term(chunk, side, target), part(ref, chunk, side), s(name, c)
            )

    def ring_stage(c):
        chunk = p, r0, n = CHUNKS[c]
        for name, make in loads(c):
            if name[0] == "n":
                make().wait()
        await_recv(part(got, chunk, 0), ("a+", c))
        await_recv(part(got, chunk, 1), ("a-", c))

        def add(t, carry):
            r = pl.ds(r0 + 4 * t, 4)
            nxt[p, r] = (nxt[p, r].astype(f32) + got[p, r].astype(f32)).astype(bf16)
            return carry

        lax.fori_loop(0, n // 4, add, 0)
        send(lambda: part(nxt, chunk, 0), lambda: part(ym, chunk, 0), ("s+", c), {"ev": e_up})
        send(lambda: part(nxt, chunk, 1), lambda: part(yp, chunk, 1), ("s-", c), {"ev": e_down})

    def ring_done(c):
        chunk = CHUNKS[c]
        for name, make in loads(c):
            if name[0] == "o":
                make().wait()
        await_recv(part(ym, chunk, 1), ("r+", c))
        await_recv(part(yp, chunk, 0), ("r-", c))
        await_recv(part(ym, chunk, 0), ("s+", c))
        await_recv(part(yp, chunk, 1), ("s-", c))

    def total_of(p, r, lanes):
        total = own[p, r, :, lanes].astype(f32) + ym[p, r, :, lanes].astype(f32)
        return total + yp[p, r, :, lanes].astype(f32)

    def lanes_of(target):
        return pl.ds(pl.multiple_of(target * block, block), block)

    def device_on_line(target):
        return {"ev": y * LINE + target}

    def pair_stage(c):
        p, r0, n = CHUNKS[c]
        rows = pl.ds(r0, n)

        def via_copy(j):
            return lambda: via_out.at[j, p, rows], lambda: via.at[j, p, rows], ("via", c, j), device_on_line(mate)

        def first():
            for j in range(2):
                lanes = lanes_of(beyond[1 - j])

                def add(t, carry):
                    r = pl.ds(r0 + 8 * t, 8)
                    via_out[j, p, r] = total_of(p, r, lanes).astype(bf16)
                    return carry

                lax.fori_loop(0, n // 8, add, 0)
                make_copy(*via_copy(j)).start()

        pl.when(at_end)(first)
        for j in range(2):
            drains.append((at_end, lambda j=j: make_copy(*via_copy(j)).wait_send()))
        lanes = lanes_of(mate)

        def add(t, carry):
            r = pl.ds(r0 + 8 * t, 8)
            near_out[p, r] = total_of(p, r, lanes)
            return carry

        lax.fori_loop(0, n // 8, add, 0)
        send(lambda: near_out.at[p, rows], lambda: near.at[p, rows], ("near", c), device_on_line(mate))

    def far_stage(c):
        p, r0, n = CHUNKS[c]
        rows = pl.ds(r0, n)

        def far_copy(j):
            to = device_on_line(beyond[j])
            return lambda: far_out.at[j, p, rows], lambda: far.at[p, rows], ("far", c), to, ("far_out", c, j)

        def second():
            for j in range(2):
                lanes = lanes_of(beyond[j])
                await_recv(via.at[j, p, rows], ("via", c, j))

                def add(t, carry):
                    r = pl.ds(r0 + 8 * t, 8)
                    far_out[j, p, r] = total_of(p, r, lanes) + via[j, p, r].astype(f32)
                    return carry

                lax.fori_loop(0, n // 8, add, 0)
                make_copy(*far_copy(j)).start()

        pl.when(inner)(second)
        for j in range(2):
            drains.append((inner, lambda j=j: make_copy(*far_copy(j)).wait_send()))

    def finish(c):
        p, r0, n = CHUNKS[c]
        zg = p % per_kernel
        rows = pl.ds(r0, n)
        lanes = pl.ds(pl.multiple_of(z * block, block), block)
        await_recv(near.at[p, rows], ("near", c))
        await_recv(far.at[p, rows], ("far", c))

        def add(t, carry):
            r = pl.ds(r0 + 8 * t, 8)
            total = total_of(p, r, lanes) + near[p, r] + far[p, r]
            cells[pl.ds(16 * PLANES * t, 16 * PLANES), :] = (total / ill[zg, r]).reshape(16 * PLANES, block)
            return carry

        lax.fori_loop(0, n // 8, add, 0)
        for side in range(2):
            for plane in range(PLANES):
                picked = cells[pl.ds(side * PLANES + plane, n, stride=2 * PLANES), :]
                xe[p, plane, 2 + side, rows, :] = picked.astype(bf16)
        src = lambda: xe.at[p, :, pl.ds(2, 2), rows, :]
        direct_up, direct_down = g < owners - 1, g > 0
        if p < pieces - 1:
            direct_up, direct_down = direct_up & (g != seam_lo), direct_down & (g != seam_hi)
            there = lambda: passed.at[:, :, rows, :]
            for name, source, to in (("u", seam_lo, by_way(p)[0]), ("v", seam_hi, by_way(p)[1])):
                send(src, there, (name, c), {"gx": jnp.int32(to)}, cond=g == source)
        send(src, lambda: xe.at[p, :, pl.ds(0, 2), rows, :], ("x+", c), {"gx": g + 1}, cond=direct_up)
        send(src, lambda: xe.at[p, :, pl.ds(4, 2), rows, :], ("x-", c), {"gx": g - 1}, cond=direct_down)

    def pass_on(c):
        p, r0, n = CHUNKS[c]
        if p == pieces - 1:
            return
        rows = pl.ds(r0, n)
        there = lambda: passed.at[:, :, rows, :]
        for name, at, to, first, arrival in (
            ("u", by_way(p)[0], seam_hi, 0, "x+"), ("v", by_way(p)[1], seam_lo, 4, "x-"),
        ):
            await_recv(there(), (name, c), g == at)
            dst = lambda first=first: xe.at[p, :, pl.ds(first, 2), rows, :]
            send(there, dst, (arrival, c), {"gx": jnp.int32(to)}, (name + "on", c), cond=g == at)

    def smooth_x(p):
        zg = p % per_kernel
        for c, (pc, r0, n) in enumerate(CHUNKS):
            if pc == p:
                await_recv(xe.at[p, :, pl.ds(0, 2), pl.ds(r0, n), :], ("x+", c), g > 0)
                await_recv(xe.at[p, :, pl.ds(4, 2), pl.ds(r0, n), :], ("x-", c), g < owners - 1)
        for a in range(0, PLANES, 2):
            data = jnp.concatenate([xe[p, b].reshape(3 * slab, block) for b in (a, a + 1)], axis=1)
            d = zg * PLANES + a
            labels = jnp.concatenate([cx_ref[d : d + 1, :], cx_ref[d + 1 : d + 2, :]], axis=1)
            product = jnp.dot(mx[...], data, preferred_element_type=f32)
            total = product[:slab]
            for level in range(1, count):
                total = jnp.where(labels == level, product[level * slab : (level + 1) * slab], total)
            bounded = (soft_bound * jnp.tanh(total / soft_bound)).astype(bf16)
            be[p, 1, a] = bounded[:, :block]
            be[p, 1, a + 1] = bounded[:, block:]
            two = pl.ds(a, 2)
            src = lambda two=two: be.at[p, 1, two]
            send(src, lambda two=two: be.at[p, 0, two], ("y+", p, a), {"ev": e + 1}, cond=e < groups - 1)
            send(src, lambda two=two: be.at[p, 2, two], ("y-", p, a), {"ev": e - 1}, cond=e > 0)

    def smooth_y(p):
        k, zg = p // per_kernel, p % per_kernel
        for a in range(0, PLANES, 2):
            two = pl.ds(a, 2)
            await_recv(be.at[p, 0, two], ("y+", p, a), e > 0)
            await_recv(be.at[p, 2, two], ("y-", p, a), e < groups - 1)
            data = jnp.concatenate([be[p, side, two].reshape(2 * slab, block) for side in range(3)], axis=1)
            product = jnp.dot(data, my[...], preferred_element_type=f32)
            deep = pl.ds(zg * PLANES + a, 2)
            labels = cyt[deep].reshape(2 * slab, block)
            total = product[:, :block]
            for level in range(1, count):
                total = jnp.where(labels == level, product[:, level * block : (level + 1) * block], total)
            out_ref[k, deep] = total.astype(out_ref.dtype).reshape(2, slab, block)

    def prepare():
        i = lax.broadcasted_iota(jnp.int32, (slab, slab + 2 * BAND), 0)
        j = lax.broadcasted_iota(jnp.int32, (slab, slab + 2 * BAND), 1)
        for level in range(count):
            mx[level * slab : (level + 1) * slab, :] = window(g * slab, slab * owners, wx_ref[level], 1, i, j)
        j = lax.broadcasted_iota(jnp.int32, (block + 2 * BAND, block), 0)
        i = lax.broadcasted_iota(jnp.int32, (block + 2 * BAND, block), 1)
        for level in range(count):
            my[:, level * block : (level + 1) * block] = window(e * block, full_y, wy_ref[level], 0, i, j)
        for plane in range(planes):
            row = cy_ref[plane : plane + 1, :].astype(f32)
            cyt[plane] = jnp.broadcast_to(row, (slab, slab)).T

        def zero(ref):
            def fill():
                ref[...] = jnp.zeros(ref.shape, ref.dtype)
            return fill

        pl.when(g == 0)(zero(xe.at[:, :, pl.ds(0, 2)]))
        pl.when(g == owners - 1)(zero(xe.at[:, :, pl.ds(4, 2)]))
        pl.when(e == 0)(zero(be.at[:, 0]))
        pl.when(e == groups - 1)(zero(be.at[:, 2]))

    def ill_loads():
        for zg in range(per_kernel):
            for side in range(2):
                yield lambda zg=zg, side=side: pltpu.make_async_copy(
                    ill_hbm.at[pl.ds(side * half, half), pl.ds(zg * PLANES, PLANES), :],
                    ill.at[zg, :, pl.ds(side * PLANES, PLANES), :], s("ill", zg, side),
                )

    chunks = len(CHUNKS)
    for c in range(chunks):
        for name, make in loads(c):
            make().start()
    for make in ill_loads():
        make().start()
    prepare()
    pl.semaphore_wait(barrier, peers)
    send_across(0)
    send_raw(0)
    send_across(1)
    ready = [max(c for c in range(chunks) if CHUNKS[c][0] == p) + 3 for p in range(pieces)]
    for slot in range(chunks + 4):
        if slot < chunks:
            ring_stage(slot)
            if slot + 1 < chunks:
                send_raw(slot + 1)
            if slot + 2 < chunks:
                send_across(slot + 2)
        if slot == 0:
            for make in ill_loads():
                make().wait()
        if 0 <= slot - 1 < chunks:
            ring_done(slot - 1)
            pair_stage(slot - 1)
        if 0 <= slot - 2 < chunks:
            finish(slot - 2)
        if 0 <= slot - 1 < chunks:
            far_stage(slot - 1)
        if 0 <= slot - 2 < chunks:
            pass_on(slot - 2)
        for p in range(pieces):
            if slot == ready[p]:
                smooth_x(p)
        for p in range(pieces):
            if slot == (ready[-1] if p == pieces - 2 else ready[p] + (1 if p == pieces - 1 else 2)):
                smooth_y(p)

    for cond, drain in drains:
        when(cond, drain)
    assert len(index) <= SEMS, len(index)


def per_device(partial_kernels, illumination, classes_x, classes_y, widths_x, widths_y):
    own_part = partial_kernels[0]
    slab, kernels, planes, full_y = own_part.shape
    groups, owners = lax.axis_size("ev"), lax.axis_size("gx")
    block = full_y // groups
    span = block * LINE
    count = widths_x.shape[0]
    pieces = kernels * planes // PLANES
    vmem, smem = pl.BlockSpec(memory_space=pltpu.VMEM), pl.BlockSpec(memory_space=pltpu.SMEM)
    hbm = pl.BlockSpec(memory_space=pl.ANY)
    wide = (pieces, slab // 2, 2 * PLANES, span)
    unit = (pieces, slab // 2, 2 * PLANES, block)
    out = pl.pallas_call(
        functools.partial(kernel, (owners, groups)),
        out_shape=jax.ShapeDtypeStruct((kernels, planes, slab, block), bf16),
        in_specs=[hbm, hbm, vmem, vmem, smem, smem],
        out_specs=vmem,
        scratch_shapes=[pltpu.VMEM(wide, bf16)] * 5
        + [pltpu.VMEM((2, *unit), bf16)] * 2
        + [pltpu.VMEM(unit, f32)] * 3
        + [
            pltpu.VMEM((2, *unit), f32),
            pltpu.VMEM((planes // PLANES, slab // 2, 2 * PLANES, block), f32),
            pltpu.VMEM((slab * PLANES, block), f32),
            pltpu.VMEM((pieces, PLANES, 6, slab // 2, block), bf16),
            pltpu.VMEM((PLANES, 2, slab // 2, block), bf16),
            pltpu.VMEM((pieces, 3, PLANES, slab, block), bf16),
            pltpu.VMEM((count * slab, slab + 2 * BAND), bf16),
            pltpu.VMEM((block + 2 * BAND, count * block), bf16),
            pltpu.VMEM((planes, slab, slab), f32),
            pltpu.SemaphoreType.DMA((SEMS,)),
        ],
        compiler_params=pltpu.CompilerParams(
            collective_id=0, has_side_effects=True, vmem_limit_bytes=56 * 1024 * 1024
        ),
        cost_estimate=pl.CostEstimate(flops=2_000_000_000, bytes_accessed=16_000_000, transcendentals=300_000),
        name="condition",
    )(own_part, illumination, classes_x, classes_y.T, widths_x, widths_y)
    return out.transpose(2, 0, 1, 3)


def solution(mesh):
    return jax.shard_map(
        per_device,
        mesh=mesh,
        in_specs=(
            P("ev", "gx", None, None, None),
            P("gx", None, "ev"),
            P(None, "ev"),
            P("gx", None),
            P(),
            P(),
        ),
        out_specs=P("gx", None, None, "ev"),
        check_vma=False,
    )
```

```python
import functools

import jax
import jax.numpy as jnp
from jax import lax
from jax.experimental import pallas as pl
from jax.experimental.pallas import tpu as pltpu
from jax.sharding import PartitionSpec as P

BAND = 128
blend_weight = 0.25
soft_bound = 2.0
MESH = pl.DeviceIdType.MESH
bf16, f32 = jnp.bfloat16, jnp.float32

RING = 4
LINE = 4
PLANES = 4
CHUNKS = ((0,0,16),(0,16,48),(1,0,32),(1,32,32),(2,0,32),(2,32,32),(3,0,32),(3,32,32))
SEMS = 420


def window(first, length, fraction, along_rows, i, j):
    offset = (i + BAND - j).astype(f32)
    source = first - BAND + j
    inside = (jnp.abs(offset) <= BAND) & (source >= 0) & (source < length)
    distance = offset / (fraction * BAND)
    gaussian = jnp.where(inside, jnp.exp(-0.5 * distance * distance), 0.0)
    gaussian = gaussian / jnp.sum(gaussian, axis=along_rows, keepdims=True)
    return (gaussian + jnp.where(offset == 0.0, blend_weight, 0.0)).astype(bf16)


def kernel(
    sizes, x_hbm, ill_hbm, cx_ref, cy_ref, wx_ref, wy_ref, out_ref,
    own, nxt, got, ym, yp, via, via_out, near, near_out, far, far_out, late, late_out, ill, cells, xe, passed, be, mx, my, cyt, sem,
):
    owners, groups = sizes
    slab, kernels, planes, full_y = x_hbm.shape
    block = full_y // groups
    span = block * LINE
    half = slab // 2
    seam_hi = owners // 2
    seam_lo = seam_hi - 1
    count = mx.shape[0] // slab
    per_kernel = planes // PLANES
    pieces = kernels * per_kernel
    g, e = lax.axis_index("gx"), lax.axis_index("ev")
    y, z = lax.div(e, LINE), lax.rem(e, LINE)
    up, down, across = (lax.rem(y + d, RING) for d in (1, RING - 1, 2))
    e_up, e_down = up * LINE + z, down * LINE + z
    mate = z + 1 - 2 * lax.rem(z, 2)
    at_end = (z == 0) | (z == LINE - 1)
    inner = jnp.logical_not(at_end)

    def by_way(p):
        return 2 * p + 1, seam_hi + 2 * (p + 1)

    beyond = (lax.rem(z + 2, LINE), lax.rem(mate + 2, LINE))

    index = {}

    def s(*key):
        return sem.at[index.setdefault(key, len(index))]

    drains = []

    def when(cond, action):
        if cond is None:
            action()
        else:
            pl.when(cond)(action)

    def make_copy(src, dst, name, to, out=None):
        return pltpu.make_async_remote_copy(
            src_ref=src(), dst_ref=dst(), send_sem=s("send", *(out or name)), recv_sem=s("recv", *name),
            device_id=to, device_id_type=MESH,
        )

    def send(*copy, cond=None):
        when(cond, lambda: make_copy(*copy).start())
        drains.append((cond, lambda: make_copy(*copy).wait_send()))

    def await_recv(dst, name, cond=None):
        when(cond, lambda: pltpu.make_async_copy(dst, dst, s("recv", *name)).wait())

    barrier = pltpu.get_barrier_semaphore()
    pl.semaphore_signal(barrier, inc=1, device_id={"ev": e_up}, device_id_type=MESH)
    pl.semaphore_signal(barrier, inc=1, device_id={"ev": e_down}, device_id_type=MESH)
    pl.semaphore_signal(barrier, inc=1, device_id={"ev": y * LINE + beyond[0]}, device_id_type=MESH)
    peers = 3
    for cond, to in (
        (e < groups - 1, {"ev": e + 1}),
        (e > 0, {"ev": e - 1}),
        (g < owners - 1, {"gx": g + 1}),
        (g > 0, {"gx": g - 1}),
    ):
        pl.when(cond)(
            functools.partial(pl.semaphore_signal, barrier, inc=1, device_id=to, device_id_type=MESH)
        )
        peers = peers + cond.astype(jnp.int32)
    for p in range(pieces - 1):
        for at, to in (
            (by_way(p)[0], seam_lo), (seam_hi, by_way(p)[0]), (by_way(p)[1], seam_hi), (seam_lo, by_way(p)[1]),
        ):
            pl.when(g == at)(
                functools.partial(pl.semaphore_signal, barrier, inc=1, device_id={"gx": to}, device_id_type=MESH)
            )
            peers = peers + (g == to).astype(jnp.int32)

    def term(chunk, side, target):
        p, r0, n = chunk
        lanes = pl.ds(pl.multiple_of(target * span, span), span)
        first = (p % per_kernel) * PLANES
        return x_hbm.at[pl.ds(side * half + r0, n), p // per_kernel, pl.ds(first, PLANES), lanes]

    def part(ref, chunk, side):
        p, r0, n = chunk
        return ref.at[p, pl.ds(r0, n), pl.ds(side * PLANES, PLANES), :]

    def send_across(c):
        chunk = CHUNKS[c]
        send(lambda: term(chunk, 0, across), lambda: part(got, chunk, 0), ("a+", c), {"ev": e_up})
        send(lambda: term(chunk, 1, across), lambda: part(got, chunk, 1), ("a-", c), {"ev": e_down})

    def send_raw(c):
        chunk = CHUNKS[c]
        send(lambda: term(chunk, 1, up), lambda: part(ym, chunk, 1), ("r+", c), {"ev": e_up})
        send(lambda: term(chunk, 0, down), lambda: part(yp, chunk, 0), ("r-", c), {"ev": e_down})

    def loads(c):
        chunk = CHUNKS[c]
        for side, ref, target, name in (
            (0, nxt, up, "n0"), (1, nxt, down, "n1"), (0, own, y, "o0"), (1, own, y, "o1"),
        ):
            yield name, lambda side=side, ref=ref, target=target, name=name: pltpu.make_async_copy(
                term(chunk, side, target), part(ref, chunk, side), s(name, c)
            )

    def ring_stage(c):
        chunk = p, r0, n = CHUNKS[c]
        for name, make in loads(c):
            if name[0] == "n":
                make().wait()
        await_recv(part(got, chunk, 0), ("a+", c))
        await_recv(part(got, chunk, 1), ("a-", c))

        def add(t, carry):
            r = pl.ds(r0 + 4 * t, 4)
            nxt[p, r] = (nxt[p, r].astype(f32) + got[p, r].astype(f32)).astype(bf16)
            return carry

        lax.fori_loop(0, n // 4, add, 0)
        send(lambda: part(nxt, chunk, 0), lambda: part(ym, chunk, 0), ("s+", c), {"ev": e_up})
        send(lambda: part(nxt, chunk, 1), lambda: part(yp, chunk, 1), ("s-", c), {"ev": e_down})

    def ring_done(c):
        chunk = CHUNKS[c]
        for name, make in loads(c):
            if name[0] == "o":
                make().wait()
        await_recv(part(ym, chunk, 1), ("r+", c))
        await_recv(part(yp, chunk, 0), ("r-", c))
        await_recv(part(ym, chunk, 0), ("s+", c))
        await_recv(part(yp, chunk, 1), ("s-", c))

    def total_of(p, r, lanes):
        total = own[p, r, :, lanes].astype(f32) + ym[p, r, :, lanes].astype(f32)
        return total + yp[p, r, :, lanes].astype(f32)

    def lanes_of(target):
        return pl.ds(pl.multiple_of(target * block, block), block)

    def device_on_line(target):
        return {"ev": y * LINE + target}

    def pair_stage(c):
        p, r0, n = CHUNKS[c]
        rows = pl.ds(r0, n)

        def via_copy(j):
            return lambda: via_out.at[j, p, rows], lambda: via.at[j, p, rows], ("via", c, j), device_on_line(mate)

        def first():
            for j in range(2):
                lanes = lanes_of(beyond[1 - j])

                def add(t, carry):
                    r = pl.ds(r0 + 8 * t, 8)
                    via_out[j, p, r] = total_of(p, r, lanes).astype(bf16)
                    return carry

                lax.fori_loop(0, n // 8, add, 0)
                make_copy(*via_copy(j)).start()

        pl.when(at_end)(first)
        for j in range(2):
            drains.append((at_end, lambda j=j: make_copy(*via_copy(j)).wait_send()))
        lanes = lanes_of(mate)

        def add(t, carry):
            r = pl.ds(r0 + 8 * t, 8)
            near_out[p, r] = total_of(p, r, lanes)
            return carry

        lax.fori_loop(0, n // 8, add, 0)
        send(lambda: near_out.at[p, rows], lambda: near.at[p, rows], ("near", c), device_on_line(mate))

    def far_stage(c):
        p, r0, n = CHUNKS[c]
        rows = pl.ds(r0, n)

        def far_copy(j):
            to = device_on_line(beyond[j])
            if c == len(CHUNKS) - 1:
                return lambda: late_out.at[j], lambda: late, ("far", c), to, ("far_out", c, j)
            return lambda: far_out.at[j, p, rows], lambda: far.at[p, rows], ("far", c), to, ("far_out", c, j)

        def second():
            for j in range(2):
                lanes = lanes_of(beyond[j])
                await_recv(via.at[j, p, rows], ("via", c, j))

                def add(t, carry):
                    r = pl.ds(r0 + 8 * t, 8)
                    total = total_of(p, r, lanes) + via[j, p, r].astype(f32)
                    if c == len(CHUNKS) - 1:
                        late_out[j, pl.ds(8 * t, 8)] = total.astype(bf16)
                    else:
                        far_out[j, p, r] = total
                    return carry

                lax.fori_loop(0, n // 8, add, 0)
                make_copy(*far_copy(j)).start()

        pl.when(inner)(second)
        for j in range(2):
            drains.append((inner, lambda j=j: make_copy(*far_copy(j)).wait_send()))

    def finish(c):
        p, r0, n = CHUNKS[c]
        zg = p % per_kernel
        rows = pl.ds(r0, n)
        lanes = pl.ds(pl.multiple_of(z * block, block), block)
        await_recv(near.at[p, rows], ("near", c))
        await_recv(late if c == len(CHUNKS) - 1 else far.at[p, rows], ("far", c))

        def add(t, carry):
            r = pl.ds(r0 + 8 * t, 8)
            beyond_pair = late[pl.ds(8 * t, 8)].astype(f32) if c == len(CHUNKS) - 1 else far[p, r]
            total = total_of(p, r, lanes) + near[p, r] + beyond_pair
            cells[pl.ds(16 * PLANES * t, 16 * PLANES), :] = (total / ill[zg, r]).reshape(16 * PLANES, block)
            return carry

        lax.fori_loop(0, n // 8, add, 0)
        for side in range(2):
            for plane in range(PLANES):
                picked = cells[pl.ds(side * PLANES + plane, n, stride=2 * PLANES), :]
                xe[p, plane, 2 + side, rows, :] = picked.astype(bf16)
        src = lambda: xe.at[p, :, pl.ds(2, 2), rows, :]
        direct_up, direct_down = g < owners - 1, g > 0
        if p < pieces - 1:
            direct_up, direct_down = direct_up & (g != seam_lo), direct_down & (g != seam_hi)
            there = lambda: passed.at[:, :, rows, :]
            for name, source, to in (("u", seam_lo, by_way(p)[0]), ("v", seam_hi, by_way(p)[1])):
                send(src, there, (name, c), {"gx": jnp.int32(to)}, cond=g == source)
        send(src, lambda: xe.at[p, :, pl.ds(0, 2), rows, :], ("x+", c), {"gx": g + 1}, cond=direct_up)
        send(src, lambda: xe.at[p, :, pl.ds(4, 2), rows, :], ("x-", c), {"gx": g - 1}, cond=direct_down)

    def pass_on(c):
        p, r0, n = CHUNKS[c]
        if p == pieces - 1:
            return
        rows = pl.ds(r0, n)
        there = lambda: passed.at[:, :, rows, :]
        for name, at, to, first, arrival in (
            ("u", by_way(p)[0], seam_hi, 0, "x+"), ("v", by_way(p)[1], seam_lo, 4, "x-"),
        ):
            await_recv(there(), (name, c), g == at)
            dst = lambda first=first: xe.at[p, :, pl.ds(first, 2), rows, :]
            send(there, dst, (arrival, c), {"gx": jnp.int32(to)}, (name + "on", c), cond=g == at)

    def smooth_x(p):
        zg = p % per_kernel
        for c, (pc, r0, n) in enumerate(CHUNKS):
            if pc == p:
                await_recv(xe.at[p, :, pl.ds(0, 2), pl.ds(r0, n), :], ("x+", c), g > 0)
                await_recv(xe.at[p, :, pl.ds(4, 2), pl.ds(r0, n), :], ("x-", c), g < owners - 1)
        for a in range(0, PLANES, 2):
            data = jnp.concatenate([xe[p, b].reshape(3 * slab, block) for b in (a, a + 1)], axis=1)
            d = zg * PLANES + a
            labels = jnp.concatenate([cx_ref[d : d + 1, :], cx_ref[d + 1 : d + 2, :]], axis=1)
            product = jnp.dot(mx[...], data, preferred_element_type=f32)
            total = product[:slab]
            for level in range(1, count):
                total = jnp.where(labels == level, product[level * slab : (level + 1) * slab], total)
            bounded = (soft_bound * jnp.tanh(total / soft_bound)).astype(bf16)
            be[p, 1, a] = bounded[:, :block]
            be[p, 1, a + 1] = bounded[:, block:]
            two = pl.ds(a, 2)
            src = lambda two=two: be.at[p, 1, two]
            send(src, lambda two=two: be.at[p, 0, two], ("y+", p, a), {"ev": e + 1}, cond=e < groups - 1)
            send(src, lambda two=two: be.at[p, 2, two], ("y-", p, a), {"ev": e - 1}, cond=e > 0)

    def smooth_y(p):
        k, zg = p // per_kernel, p % per_kernel
        for a in range(0, PLANES, 2):
            two = pl.ds(a, 2)
            await_recv(be.at[p, 0, two], ("y+", p, a), e > 0)
            await_recv(be.at[p, 2, two], ("y-", p, a), e < groups - 1)
            data = jnp.concatenate([be[p, side, two].reshape(2 * slab, block) for side in range(3)], axis=1)
            product = jnp.dot(data, my[...], preferred_element_type=f32)
            deep = pl.ds(zg * PLANES + a, 2)
            labels = cyt[deep].reshape(2 * slab, block)
            total = product[:, :block]
            for level in range(1, count):
                total = jnp.where(labels == level, product[:, level * block : (level + 1) * block], total)
            out_ref[k, deep] = total.astype(out_ref.dtype).reshape(2, slab, block)

    def prepare():
        i = lax.broadcasted_iota(jnp.int32, (slab, slab + 2 * BAND), 0)
        j = lax.broadcasted_iota(jnp.int32, (slab, slab + 2 * BAND), 1)
        for level in range(count):
            mx[level * slab : (level + 1) * slab, :] = window(g * slab, slab * owners, wx_ref[level], 1, i, j)
        j = lax.broadcasted_iota(jnp.int32, (block + 2 * BAND, block), 0)
        i = lax.broadcasted_iota(jnp.int32, (block + 2 * BAND, block), 1)
        for level in range(count):
            my[:, level * block : (level + 1) * block] = window(e * block, full_y, wy_ref[level], 0, i, j)
        for plane in range(planes):
            row = cy_ref[plane : plane + 1, :].astype(f32)
            cyt[plane] = jnp.broadcast_to(row, (slab, slab)).T

        def zero(ref):
            def fill():
                ref[...] = jnp.zeros(ref.shape, ref.dtype)
            return fill

        pl.when(g == 0)(zero(xe.at[:, :, pl.ds(0, 2)]))
        pl.when(g == owners - 1)(zero(xe.at[:, :, pl.ds(4, 2)]))
        pl.when(e == 0)(zero(be.at[:, 0]))
        pl.when(e == groups - 1)(zero(be.at[:, 2]))

    def ill_loads():
        for zg in range(per_kernel):
            for side in range(2):
                yield lambda zg=zg, side=side: pltpu.make_async_copy(
                    ill_hbm.at[pl.ds(side * half, half), pl.ds(zg * PLANES, PLANES), :],
                    ill.at[zg, :, pl.ds(side * PLANES, PLANES), :], s("ill", zg, side),
                )

    chunks = len(CHUNKS)
    for c in range(chunks):
        for name, make in loads(c):
            make().start()
    for make in ill_loads():
        make().start()
    prepare()
    pl.semaphore_wait(barrier, peers)
    send_across(0)
    send_raw(0)
    send_across(1)
    last = [max(c for c in range(chunks) if CHUNKS[c][0] == p) for p in range(pieces)]
    ready = [last[p] + (3, 3, 4, 3)[p] for p in range(pieces)]
    for slot in range(chunks + 4):
        if slot < chunks:
            ring_stage(slot)
            if slot + 1 < chunks:
                send_raw(slot + 1)
            if slot + 2 < chunks:
                send_across(slot + 2)
        if slot == 0:
            for make in ill_loads():
                make().wait()
        if 0 <= slot - 1 < chunks:
            ring_done(slot - 1)
            pair_stage(slot - 1)
        if 0 <= slot - 2 < chunks:
            finish(slot - 2)
        if 0 <= slot - 1 < chunks:
            far_stage(slot - 1)
        if 0 <= slot - 2 < chunks:
            pass_on(slot - 2)
        for p in range(pieces):
            if slot == ready[p]:
                smooth_x(p)
        for p in range(pieces):
            if slot == ready[-1] + (1 if p == pieces - 1 else 0):
                smooth_y(p)

    for cond, drain in drains:
        when(cond, drain)
    assert len(index) <= SEMS, len(index)


def per_device(partial_kernels, illumination, classes_x, classes_y, widths_x, widths_y):
    own_part = partial_kernels[0]
    slab, kernels, planes, full_y = own_part.shape
    groups, owners = lax.axis_size("ev"), lax.axis_size("gx")
    block = full_y // groups
    span = block * LINE
    count = widths_x.shape[0]
    pieces = kernels * planes // PLANES
    vmem, smem = pl.BlockSpec(memory_space=pltpu.VMEM), pl.BlockSpec(memory_space=pltpu.SMEM)
    hbm = pl.BlockSpec(memory_space=pl.ANY)
    wide = (pieces, slab // 2, 2 * PLANES, span)
    unit = (pieces, slab // 2, 2 * PLANES, block)
    out = pl.pallas_call(
        functools.partial(kernel, (owners, groups)),
        out_shape=jax.ShapeDtypeStruct((kernels, planes, slab, block), bf16),
        in_specs=[hbm, hbm, vmem, vmem, smem, smem],
        out_specs=vmem,
        scratch_shapes=[pltpu.VMEM(wide, bf16)] * 5
        + [pltpu.VMEM((2, *unit), bf16)] * 2
        + [pltpu.VMEM(unit, f32)] * 3
        + [
            pltpu.VMEM((2, *unit), f32),
            pltpu.VMEM((CHUNKS[-1][2], *unit[2:]), bf16),
            pltpu.VMEM((2, CHUNKS[-1][2], *unit[2:]), bf16),
            pltpu.VMEM((planes // PLANES, slab // 2, 2 * PLANES, block), f32),
            pltpu.VMEM((slab * PLANES, block), f32),
            pltpu.VMEM((pieces, PLANES, 6, slab // 2, block), bf16),
            pltpu.VMEM((PLANES, 2, slab // 2, block), bf16),
            pltpu.VMEM((pieces, 3, PLANES, slab, block), bf16),
            pltpu.VMEM((count * slab, slab + 2 * BAND), bf16),
            pltpu.VMEM((block + 2 * BAND, count * block), bf16),
            pltpu.VMEM((planes, slab, slab), f32),
            pltpu.SemaphoreType.DMA((SEMS,)),
        ],
        compiler_params=pltpu.CompilerParams(
            collective_id=0, has_side_effects=True, vmem_limit_bytes=56 * 1024 * 1024
        ),
        cost_estimate=pl.CostEstimate(flops=2_000_000_000, bytes_accessed=16_000_000, transcendentals=300_000),
        name="condition",
    )(own_part, illumination, classes_x, classes_y.T, widths_x, widths_y)
    return out.transpose(2, 0, 1, 3)


def solution(mesh):
    return jax.shard_map(
        per_device,
        mesh=mesh,
        in_specs=(
            P("ev", "gx", None, None, None),
            P("gx", None, "ev"),
            P(None, "ev"),
            P("gx", None),
            P(),
            P(),
        ),
        out_specs=P("gx", None, None, "ev"),
        check_vma=False,
    )
```

```python
import functools

import jax
import jax.numpy as jnp
from jax import lax
from jax.experimental import pallas as pl
from jax.experimental.pallas import tpu as pltpu
from jax.sharding import PartitionSpec as P

BAND = 128
blend_weight = 0.25
soft_bound = 2.0
MESH = pl.DeviceIdType.MESH
bf16, f32 = jnp.bfloat16, jnp.float32

RING = 4
LINE = 4
PLANES = 4
CHUNKS = ((0,0,16),(0,16,48),(1,0,32),(1,32,32),(2,0,32),(2,32,32),(3,0,32),(3,32,32))
SEMS = 420


def window(first, length, fraction, along_rows, i, j):
    offset = (i + BAND - j).astype(f32)
    source = first - BAND + j
    inside = (jnp.abs(offset) <= BAND) & (source >= 0) & (source < length)
    distance = offset / (fraction * BAND)
    gaussian = jnp.where(inside, jnp.exp(-0.5 * distance * distance), 0.0)
    gaussian = gaussian / jnp.sum(gaussian, axis=along_rows, keepdims=True)
    return (gaussian + jnp.where(offset == 0.0, blend_weight, 0.0)).astype(bf16)


def kernel(
    sizes, x_hbm, ill_hbm, cx_ref, cy_ref, wx_ref, wy_ref, out_ref,
    own, nxt, got, ym, yp, via, via_out, near, near_out, far, far_out, late, late_out, ill, cells, xe, passed, be, mx, my, cyt, outs, sem,
):
    owners, groups = sizes
    slab, kernels, planes, full_y = x_hbm.shape
    block = full_y // groups
    span = block * LINE
    half = slab // 2
    seam_hi = owners // 2
    seam_lo = seam_hi - 1
    count = mx.shape[0] // slab
    per_kernel = planes // PLANES
    pieces = kernels * per_kernel
    g, e = lax.axis_index("gx"), lax.axis_index("ev")
    y, z = lax.div(e, LINE), lax.rem(e, LINE)
    up, down, across = (lax.rem(y + d, RING) for d in (1, RING - 1, 2))
    e_up, e_down = up * LINE + z, down * LINE + z
    mate = z + 1 - 2 * lax.rem(z, 2)
    at_end = (z == 0) | (z == LINE - 1)
    inner = jnp.logical_not(at_end)

    def by_way(p):
        return 2 * p + 1, seam_hi + 2 * (p + 1)

    beyond = (lax.rem(z + 2, LINE), lax.rem(mate + 2, LINE))

    index = {}

    def s(*key):
        return sem.at[index.setdefault(key, len(index))]

    drains = []

    def when(cond, action):
        if cond is None:
            action()
        else:
            pl.when(cond)(action)

    def make_copy(src, dst, name, to, out=None):
        return pltpu.make_async_remote_copy(
            src_ref=src(), dst_ref=dst(), send_sem=s("send", *(out or name)), recv_sem=s("recv", *name),
            device_id=to, device_id_type=MESH,
        )

    def send(*copy, cond=None):
        when(cond, lambda: make_copy(*copy).start())
        drains.append((cond, lambda: make_copy(*copy).wait_send()))

    def await_recv(dst, name, cond=None):
        when(cond, lambda: pltpu.make_async_copy(dst, dst, s("recv", *name)).wait())

    barrier = pltpu.get_barrier_semaphore()
    pl.semaphore_signal(barrier, inc=1, device_id={"ev": e_up}, device_id_type=MESH)
    pl.semaphore_signal(barrier, inc=1, device_id={"ev": e_down}, device_id_type=MESH)
    pl.semaphore_signal(barrier, inc=1, device_id={"ev": y * LINE + beyond[0]}, device_id_type=MESH)
    peers = 3
    for cond, to in (
        (e < groups - 1, {"ev": e + 1}),
        (e > 0, {"ev": e - 1}),
        (g < owners - 1, {"gx": g + 1}),
        (g > 0, {"gx": g - 1}),
    ):
        pl.when(cond)(
            functools.partial(pl.semaphore_signal, barrier, inc=1, device_id=to, device_id_type=MESH)
        )
        peers = peers + cond.astype(jnp.int32)
    for p in range(pieces - 1):
        for at, to in (
            (by_way(p)[0], seam_lo), (seam_hi, by_way(p)[0]), (by_way(p)[1], seam_hi), (seam_lo, by_way(p)[1]),
        ):
            pl.when(g == at)(
                functools.partial(pl.semaphore_signal, barrier, inc=1, device_id={"gx": to}, device_id_type=MESH)
            )
            peers = peers + (g == to).astype(jnp.int32)

    def term(chunk, side, target):
        p, r0, n = chunk
        lanes = pl.ds(pl.multiple_of(target * span, span), span)
        first = (p % per_kernel) * PLANES
        return x_hbm.at[pl.ds(side * half + r0, n), p // per_kernel, pl.ds(first, PLANES), lanes]

    def part(ref, chunk, side):
        p, r0, n = chunk
        return ref.at[p, pl.ds(r0, n), pl.ds(side * PLANES, PLANES), :]

    def send_across(c):
        chunk = CHUNKS[c]
        send(lambda: term(chunk, 0, across), lambda: part(got, chunk, 0), ("a+", c), {"ev": e_up})
        send(lambda: term(chunk, 1, across), lambda: part(got, chunk, 1), ("a-", c), {"ev": e_down})

    def send_raw(c):
        chunk = CHUNKS[c]
        send(lambda: term(chunk, 1, up), lambda: part(ym, chunk, 1), ("r+", c), {"ev": e_up})
        send(lambda: term(chunk, 0, down), lambda: part(yp, chunk, 0), ("r-", c), {"ev": e_down})

    def loads(c):
        chunk = CHUNKS[c]
        for side, ref, target, name in (
            (0, nxt, up, "n0"), (1, nxt, down, "n1"), (0, own, y, "o0"), (1, own, y, "o1"),
        ):
            yield name, lambda side=side, ref=ref, target=target, name=name: pltpu.make_async_copy(
                term(chunk, side, target), part(ref, chunk, side), s(name, c)
            )

    def ring_stage(c):
        chunk = p, r0, n = CHUNKS[c]
        for name, make in loads(c):
            if name[0] == "n":
                make().wait()
        await_recv(part(got, chunk, 0), ("a+", c))
        await_recv(part(got, chunk, 1), ("a-", c))

        def add(t, carry):
            r = pl.ds(r0 + 4 * t, 4)
            nxt[p, r] = (nxt[p, r].astype(f32) + got[p, r].astype(f32)).astype(bf16)
            return carry

        lax.fori_loop(0, n // 4, add, 0)
        send(lambda: part(nxt, chunk, 0), lambda: part(ym, chunk, 0), ("s+", c), {"ev": e_up})
        send(lambda: part(nxt, chunk, 1), lambda: part(yp, chunk, 1), ("s-", c), {"ev": e_down})

    def ring_done(c):
        chunk = CHUNKS[c]
        for name, make in loads(c):
            if name[0] == "o":
                make().wait()
        await_recv(part(ym, chunk, 1), ("r+", c))
        await_recv(part(yp, chunk, 0), ("r-", c))
        await_recv(part(ym, chunk, 0), ("s+", c))
        await_recv(part(yp, chunk, 1), ("s-", c))

    def total_of(p, r, lanes):
        total = own[p, r, :, lanes].astype(f32) + ym[p, r, :, lanes].astype(f32)
        return total + yp[p, r, :, lanes].astype(f32)

    def lanes_of(target):
        return pl.ds(pl.multiple_of(target * block, block), block)

    def device_on_line(target):
        return {"ev": y * LINE + target}

    def pair_stage(c):
        p, r0, n = CHUNKS[c]
        rows = pl.ds(r0, n)

        def via_copy(j):
            return lambda: via_out.at[j, p, rows], lambda: via.at[j, p, rows], ("via", c, j), device_on_line(mate)

        def first():
            for j in range(2):
                lanes = lanes_of(beyond[1 - j])

                def add(t, carry):
                    r = pl.ds(r0 + 8 * t, 8)
                    via_out[j, p, r] = total_of(p, r, lanes).astype(bf16)
                    return carry

                lax.fori_loop(0, n // 8, add, 0)
                make_copy(*via_copy(j)).start()

        pl.when(at_end)(first)
        for j in range(2):
            drains.append((at_end, lambda j=j: make_copy(*via_copy(j)).wait_send()))
        lanes = lanes_of(mate)

        def add(t, carry):
            r = pl.ds(r0 + 8 * t, 8)
            near_out[p, r] = total_of(p, r, lanes)
            return carry

        lax.fori_loop(0, n // 8, add, 0)
        send(lambda: near_out.at[p, rows], lambda: near.at[p, rows], ("near", c), device_on_line(mate))

    def far_stage(c):
        p, r0, n = CHUNKS[c]
        rows = pl.ds(r0, n)

        def far_copy(j):
            to = device_on_line(beyond[j])
            if c == len(CHUNKS) - 1:
                return lambda: late_out.at[j], lambda: late, ("far", c), to, ("far_out", c, j)
            return lambda: far_out.at[j, p, rows], lambda: far.at[p, rows], ("far", c), to, ("far_out", c, j)

        def second():
            for j in range(2):
                lanes = lanes_of(beyond[j])
                await_recv(via.at[j, p, rows], ("via", c, j))

                def add(t, carry):
                    r = pl.ds(r0 + 8 * t, 8)
                    total = total_of(p, r, lanes) + via[j, p, r].astype(f32)
                    if c == len(CHUNKS) - 1:
                        late_out[j, pl.ds(8 * t, 8)] = total.astype(bf16)
                    else:
                        far_out[j, p, r] = total
                    return carry

                lax.fori_loop(0, n // 8, add, 0)
                make_copy(*far_copy(j)).start()

        pl.when(inner)(second)
        for j in range(2):
            drains.append((inner, lambda j=j: make_copy(*far_copy(j)).wait_send()))

    def finish(c):
        p, r0, n = CHUNKS[c]
        zg = p % per_kernel
        rows = pl.ds(r0, n)
        lanes = pl.ds(pl.multiple_of(z * block, block), block)
        await_recv(near.at[p, rows], ("near", c))
        await_recv(late if c == len(CHUNKS) - 1 else far.at[p, rows], ("far", c))

        def add(t, carry):
            r = pl.ds(r0 + 8 * t, 8)
            beyond_pair = late[pl.ds(8 * t, 8)].astype(f32) if c == len(CHUNKS) - 1 else far[p, r]
            total = total_of(p, r, lanes) + near[p, r] + beyond_pair
            cells[pl.ds(16 * PLANES * t, 16 * PLANES), :] = (total / ill[zg, r]).reshape(16 * PLANES, block)
            return carry

        lax.fori_loop(0, n // 8, add, 0)
        for side in range(2):
            for plane in range(PLANES):
                picked = cells[pl.ds(side * PLANES + plane, n, stride=2 * PLANES), :]
                xe[p, plane, 2 + side, rows, :] = picked.astype(bf16)
        src = lambda: xe.at[p, :, pl.ds(2, 2), rows, :]
        direct_up, direct_down = g < owners - 1, g > 0
        if p < pieces - 1:
            direct_up, direct_down = direct_up & (g != seam_lo), direct_down & (g != seam_hi)
            there = lambda: passed.at[:, :, rows, :]
            for name, source, to in (("u", seam_lo, by_way(p)[0]), ("v", seam_hi, by_way(p)[1])):
                send(src, there, (name, c), {"gx": jnp.int32(to)}, cond=g == source)
        send(src, lambda: xe.at[p, :, pl.ds(0, 2), rows, :], ("x+", c), {"gx": g + 1}, cond=direct_up)
        send(src, lambda: xe.at[p, :, pl.ds(4, 2), rows, :], ("x-", c), {"gx": g - 1}, cond=direct_down)

    def pass_on(c):
        p, r0, n = CHUNKS[c]
        if p == pieces - 1:
            return
        rows = pl.ds(r0, n)
        there = lambda: passed.at[:, :, rows, :]
        for name, at, to, first, arrival in (
            ("u", by_way(p)[0], seam_hi, 0, "x+"), ("v", by_way(p)[1], seam_lo, 4, "x-"),
        ):
            await_recv(there(), (name, c), g == at)
            dst = lambda first=first: xe.at[p, :, pl.ds(first, 2), rows, :]
            send(there, dst, (arrival, c), {"gx": jnp.int32(to)}, (name + "on", c), cond=g == at)

    def smooth_x(p):
        zg = p % per_kernel
        for c, (pc, r0, n) in enumerate(CHUNKS):
            if pc == p:
                await_recv(xe.at[p, :, pl.ds(0, 2), pl.ds(r0, n), :], ("x+", c), g > 0)
                await_recv(xe.at[p, :, pl.ds(4, 2), pl.ds(r0, n), :], ("x-", c), g < owners - 1)
        for a in range(0, PLANES, 2):
            data = jnp.concatenate([xe[p, b].reshape(3 * slab, block) for b in (a, a + 1)], axis=1)
            d = zg * PLANES + a
            labels = jnp.concatenate([cx_ref[d : d + 1, :], cx_ref[d + 1 : d + 2, :]], axis=1)
            product = jnp.dot(mx[...], data, preferred_element_type=f32)
            total = product[:slab]
            for level in range(1, count):
                total = jnp.where(labels == level, product[level * slab : (level + 1) * slab], total)
            bounded = (soft_bound * jnp.tanh(total / soft_bound)).astype(bf16)
            be[p, 1, a] = bounded[:, :block]
            be[p, 1, a + 1] = bounded[:, block:]
            two = pl.ds(a, 2)
            src = lambda two=two: be.at[p, 1, two]
            send(src, lambda two=two: be.at[p, 0, two], ("y+", p, a), {"ev": e + 1}, cond=e < groups - 1)
            send(src, lambda two=two: be.at[p, 2, two], ("y-", p, a), {"ev": e - 1}, cond=e > 0)

    def smooth_y(p):
        k, zg = p // per_kernel, p % per_kernel
        for a in range(0, PLANES, 2):
            two = pl.ds(a, 2)
            await_recv(be.at[p, 0, two], ("y+", p, a), e > 0)
            await_recv(be.at[p, 2, two], ("y-", p, a), e < groups - 1)
            data = jnp.concatenate([be[p, side, two].reshape(2 * slab, block) for side in range(3)], axis=1)
            product = jnp.dot(data, my[...], preferred_element_type=f32)
            deep = pl.ds(zg * PLANES + a, 2)
            labels = cyt[deep].reshape(2 * slab, block)
            total = product[:, :block]
            for level in range(1, count):
                total = jnp.where(labels == level, product[:, level * block : (level + 1) * block], total)
            for b in range(2):
                cells[pl.ds(a + b, slab, stride=PLANES), :] = total[b * slab : (b + 1) * slab]
        outs[p] = cells[...].reshape(slab, PLANES, block).astype(outs.dtype)
        out_copy(p).start()

    def out_copy(p):
        k, zg = p // per_kernel, p % per_kernel
        return pltpu.make_async_copy(outs.at[p], out_ref.at[:, k, pl.ds(zg * PLANES, PLANES), :], s("out", p))

    def prepare():
        i = lax.broadcasted_iota(jnp.int32, (slab, slab + 2 * BAND), 0)
        j = lax.broadcasted_iota(jnp.int32, (slab, slab + 2 * BAND), 1)
        for level in range(count):
            mx[level * slab : (level + 1) * slab, :] = window(g * slab, slab * owners, wx_ref[level], 1, i, j)
        j = lax.broadcasted_iota(jnp.int32, (block + 2 * BAND, block), 0)
        i = lax.broadcasted_iota(jnp.int32, (block + 2 * BAND, block), 1)
        for level in range(count):
            my[:, level * block : (level + 1) * block] = window(e * block, full_y, wy_ref[level], 0, i, j)
        for plane in range(planes):
            row = cy_ref[plane : plane + 1, :].astype(f32)
            cyt[plane] = jnp.broadcast_to(row, (slab, slab)).T

        def zero(ref):
            def fill():
                ref[...] = jnp.zeros(ref.shape, ref.dtype)
            return fill

        pl.when(g == 0)(zero(xe.at[:, :, pl.ds(0, 2)]))
        pl.when(g == owners - 1)(zero(xe.at[:, :, pl.ds(4, 2)]))
        pl.when(e == 0)(zero(be.at[:, 0]))
        pl.when(e == groups - 1)(zero(be.at[:, 2]))

    def ill_loads():
        for zg in range(per_kernel):
            for side in range(2):
                yield lambda zg=zg, side=side: pltpu.make_async_copy(
                    ill_hbm.at[pl.ds(side * half, half), pl.ds(zg * PLANES, PLANES), :],
                    ill.at[zg, :, pl.ds(side * PLANES, PLANES), :], s("ill", zg, side),
                )

    chunks = len(CHUNKS)
    for c in range(chunks):
        for name, make in loads(c):
            make().start()
    for make in ill_loads():
        make().start()
    prepare()
    pl.semaphore_wait(barrier, peers)
    send_across(0)
    send_raw(0)
    send_across(1)
    last = [max(c for c in range(chunks) if CHUNKS[c][0] == p) for p in range(pieces)]
    ready = [last[p] + (3, 3, 4, 3)[p] for p in range(pieces)]
    for slot in range(chunks + 4):
        if slot < chunks:
            ring_stage(slot)
            if slot + 1 < chunks:
                send_raw(slot + 1)
            if slot + 2 < chunks:
                send_across(slot + 2)
        if slot == 0:
            for make in ill_loads():
                make().wait()
        if 0 <= slot - 1 < chunks:
            ring_done(slot - 1)
            pair_stage(slot - 1)
        if 0 <= slot - 2 < chunks:
            finish(slot - 2)
        if 0 <= slot - 1 < chunks:
            far_stage(slot - 1)
        if 0 <= slot - 2 < chunks:
            pass_on(slot - 2)
        for p in range(pieces):
            if slot == ready[p]:
                smooth_x(p)
        for p in range(pieces):
            if slot == ready[-1] + (1 if p == pieces - 1 else 0):
                smooth_y(p)

    for p in range(pieces):
        out_copy(p).wait()
    for cond, drain in drains:
        when(cond, drain)
    assert len(index) <= SEMS, len(index)


def per_device(partial_kernels, illumination, classes_x, classes_y, widths_x, widths_y):
    own_part = partial_kernels[0]
    slab, kernels, planes, full_y = own_part.shape
    groups, owners = lax.axis_size("ev"), lax.axis_size("gx")
    block = full_y // groups
    span = block * LINE
    count = widths_x.shape[0]
    pieces = kernels * planes // PLANES
    vmem, smem = pl.BlockSpec(memory_space=pltpu.VMEM), pl.BlockSpec(memory_space=pltpu.SMEM)
    hbm = pl.BlockSpec(memory_space=pl.ANY)
    wide = (pieces, slab // 2, 2 * PLANES, span)
    unit = (pieces, slab // 2, 2 * PLANES, block)
    return pl.pallas_call(
        functools.partial(kernel, (owners, groups)),
        out_shape=jax.ShapeDtypeStruct((slab, kernels, planes, block), bf16),
        in_specs=[hbm, hbm, vmem, vmem, smem, smem],
        out_specs=hbm,
        scratch_shapes=[pltpu.VMEM(wide, bf16)] * 5
        + [pltpu.VMEM((2, *unit), bf16)] * 2
        + [pltpu.VMEM(unit, f32)] * 3
        + [
            pltpu.VMEM((2, *unit), f32),
            pltpu.VMEM((CHUNKS[-1][2], *unit[2:]), bf16),
            pltpu.VMEM((2, CHUNKS[-1][2], *unit[2:]), bf16),
            pltpu.VMEM((planes // PLANES, slab // 2, 2 * PLANES, block), f32),
            pltpu.VMEM((slab * PLANES, block), f32),
            pltpu.VMEM((pieces, PLANES, 6, slab // 2, block), bf16),
            pltpu.VMEM((PLANES, 2, slab // 2, block), bf16),
            pltpu.VMEM((pieces, 3, PLANES, slab, block), bf16),
            pltpu.VMEM((count * slab, slab + 2 * BAND), bf16),
            pltpu.VMEM((block + 2 * BAND, count * block), bf16),
            pltpu.VMEM((planes, slab, slab), f32),
            pltpu.VMEM((pieces, slab, PLANES, block), bf16),
            pltpu.SemaphoreType.DMA((SEMS,)),
        ],
        compiler_params=pltpu.CompilerParams(
            collective_id=0, has_side_effects=True, vmem_limit_bytes=56 * 1024 * 1024
        ),
        cost_estimate=pl.CostEstimate(flops=2_000_000_000, bytes_accessed=16_000_000, transcendentals=300_000),
        name="condition",
    )(own_part, illumination, classes_x, classes_y.T, widths_x, widths_y)


def solution(mesh):
    return jax.shard_map(
        per_device,
        mesh=mesh,
        in_specs=(
            P("ev", "gx", None, None, None),
            P("gx", None, "ev"),
            P(None, "ev"),
            P("gx", None),
            P(),
            P(),
        ),
        out_specs=P("gx", None, None, "ev"),
        check_vma=False,
    )
```
